8 devices in a mesh: dp: 1 (over z), ep: 8 (over y, x, core).
Axes of the slice: x: 2, y: 2, z: 1, core: 2. Of those that a mesh axis runs over, the one named last changes fastest.
Arguments:
- hidden_in: bfloat16 [1536, 2048], P(('dp', 'ep'))
- norm_gain: float32 [2048], replicated
- router_w: float32 [64, 2048], replicated
- w_gate: bfloat16 [64, 2048, 1408], P('ep')
- w_up: bfloat16 [64, 2048, 1408], P('ep')
- w_down: bfloat16 [64, 1408, 2048], P('ep')
- ws_gate: bfloat16 [2048, 2816], replicated
- ws_up: bfloat16 [2048, 2816], replicated
- ws_down: bfloat16 [2816, 2048], replicated
- expert_ids: int32 [1536, 6], P(('dp', 'ep'))
Outputs:
- output: bfloat16 [1536, 2048], P(('dp', 'ep'))
All inputs are finite; a program needn't handle non-finite values.
Results may differ from the reference program's by a relative error of at most 0.00436671.
Values are sent between devices in bfloat16 or wider.
A program may use at most 1 GiB of HBM per device.

```python
import jax
import jax.numpy as jnp
from jax import lax

TOKENS = 1536
D = 2048
EXPERTS = 64
INTER = 1408
SHARED_INTER = 2816
TOP = 6
GROUPS = 8
GROUP_LIMIT = 4

NORM_EPS = 1e-6
ROUTE_SCALE = 2.5
GROUP_WIDTH = EXPERTS // GROUPS
SLOT_PAIRS = (TOP + GROUP_LIMIT - 1) // GROUP_LIMIT
EXP_CAP = GROUPS * SLOT_PAIRS * TOKENS // EXPERTS


def draw_routes(route_key):
    key_hot, key_other, key_shift, key_cols = jax.random.split(route_key, 4)
    slot_sizes = [TOP // GROUP_LIMIT + int(slot_num < TOP % GROUP_LIMIT) for slot_num in range(GROUP_LIMIT)]
    slot_of_pair = jnp.array([slot_num for slot_num in range(GROUP_LIMIT) for step_num in range(slot_sizes[slot_num])], jnp.int32)
    step_of_pair = jnp.array([step_num for slot_num in range(GROUP_LIMIT) for step_num in range(slot_sizes[slot_num])], jnp.int32)
    hot_group = jax.random.randint(key_hot, (), 0, GROUPS).astype(jnp.int32)
    other_scores = jax.random.randint(key_other, (TOKENS, GROUPS - 1), 0, 1 << 20).astype(jnp.int32) * (GROUPS - 1) + jnp.arange(GROUPS - 1, dtype=jnp.int32)
    other_offsets = jnp.argsort(other_scores, axis=1)[:, : GROUP_LIMIT - 1].astype(jnp.int32)
    token_groups = jnp.concatenate([jnp.zeros((TOKENS, 1), jnp.int32) + hot_group, (hot_group + 1 + other_offsets) % GROUPS], axis=1)
    pair_groups = token_groups[:, slot_of_pair]
    group_shift = jax.random.randint(key_shift, (GROUPS,), 0, GROUP_WIDTH).astype(jnp.int32)
    token_pos = jnp.arange(TOKENS, dtype=jnp.int32)[:, None]
    within = (token_pos + step_of_pair[None, :] + group_shift[pair_groups]) % GROUP_WIDTH
    routes = pair_groups * GROUP_WIDTH + within
    col_scores = jax.random.randint(key_cols, (TOKENS, TOP), 0, 1 << 20).astype(jnp.int32) * TOP + jnp.arange(TOP, dtype=jnp.int32)
    col_order = jnp.argsort(col_scores, axis=1)
    return jnp.take_along_axis(routes, col_order, axis=1).astype(jnp.int32)


def setup_inputs(seed: int = 0, part: int = 0) -> dict:
    base_key = jax.random.key(seed)
    weight_keys = jax.random.split(base_key, 9)
    part_keys = jax.random.split(jax.random.fold_in(base_key, part), 2)
    hidden_in = jax.random.normal(part_keys[0], (TOKENS, D), jnp.float32).astype(jnp.bfloat16)
    expert_ids = draw_routes(part_keys[1])
    norm_gain = jax.random.uniform(weight_keys[0], (D,), jnp.float32, 0.5, 1.5)
    router_w = jax.random.normal(weight_keys[1], (EXPERTS, D), jnp.float32) * D ** -0.5
    w_gate = (jax.random.normal(weight_keys[2], (EXPERTS, D, INTER), jnp.float32) * D ** -0.5).astype(jnp.bfloat16)
    w_up = (jax.random.normal(weight_keys[3], (EXPERTS, D, INTER), jnp.float32) * D ** -0.5).astype(jnp.bfloat16)
    out_scale = jax.random.uniform(weight_keys[4], (EXPERTS, 1, 1), jnp.float32, 1.0, 3.0)
    w_down = (jax.random.normal(weight_keys[5], (EXPERTS, INTER, D), jnp.float32) * INTER ** -0.5 * out_scale).astype(jnp.bfloat16)
    ws_gate = (jax.random.normal(weight_keys[6], (D, SHARED_INTER), jnp.float32) * D ** -0.5).astype(jnp.bfloat16)
    ws_up = (jax.random.normal(weight_keys[7], (D, SHARED_INTER), jnp.float32) * D ** -0.5).astype(jnp.bfloat16)
    ws_down = (jax.random.normal(weight_keys[8], (SHARED_INTER, D), jnp.float32) * SHARED_INTER ** -0.5).astype(jnp.bfloat16)
    return {"hidden_in": hidden_in, "norm_gain": norm_gain, "router_w": router_w, "w_gate": w_gate, "w_up": w_up, "w_down": w_down, "ws_gate": ws_gate, "ws_up": ws_up, "ws_down": ws_down, "expert_ids": expert_ids}


def swiglu(tok_rows, gate_mat, up_mat, down_mat):
    h_gate = jnp.dot(tok_rows, gate_mat, preferred_element_type=jnp.float32)
    h_up = jnp.dot(tok_rows, up_mat, preferred_element_type=jnp.float32)
    hidden = (jax.nn.silu(h_gate) * h_up).astype(jnp.bfloat16)
    return jnp.dot(hidden, down_mat, preferred_element_type=jnp.float32).astype(jnp.bfloat16)


def reference(hidden_in, norm_gain, router_w, w_gate, w_up, w_down, ws_gate, ws_up, ws_down, expert_ids):
    x_f32 = hidden_in.astype(jnp.float32)
    inv_rms = lax.rsqrt(jnp.mean(x_f32 * x_f32, axis=1, keepdims=True) + NORM_EPS)
    x_norm = (x_f32 * inv_rms * norm_gain).astype(jnp.bfloat16)
    scores = jax.nn.sigmoid(jnp.dot(x_norm.astype(jnp.float32), router_w.T))
    picked = jnp.take_along_axis(scores, expert_ids, axis=1)
    gate_vals = ROUTE_SCALE * picked / jnp.sum(picked, axis=1, keepdims=True)
    flat_ids = expert_ids.reshape(-1)
    pair_tok = jnp.arange(TOKENS * TOP, dtype=jnp.int32) // TOP
    sort_order = jnp.argsort(flat_ids)
    counts = jnp.bincount(flat_ids, length=EXPERTS).astype(jnp.int32)
    starts = jnp.cumsum(counts) - counts
    sorted_tok = jnp.concatenate([pair_tok[sort_order], jnp.full((EXP_CAP,), TOKENS, jnp.int32)])
    norm_pad = jnp.concatenate([x_norm, jnp.zeros((1, D), x_norm.dtype)], axis=0)

    def one_expert(expert_xs):
        gate_mat, up_mat, down_mat, row_start, row_count = expert_xs
        row_tok = lax.dynamic_slice(sorted_tok, (row_start,), (EXP_CAP,))
        row_tok = jnp.where(jnp.arange(EXP_CAP, dtype=jnp.int32) < row_count, row_tok, TOKENS)
        return swiglu(norm_pad[row_tok], gate_mat, up_mat, down_mat)

    expert_out = lax.map(one_expert, (w_gate, w_up, w_down, starts, counts))
    sorted_rank = (jnp.arange(TOKENS * TOP, dtype=jnp.int32) - starts[flat_ids[sort_order]]).astype(jnp.int32)
    pair_rank = jnp.zeros((TOKENS * TOP,), jnp.int32).at[sort_order].set(sorted_rank)
    pair_out = expert_out[flat_ids, pair_rank].reshape(TOKENS, TOP, D)
    routed = jnp.sum(gate_vals[:, :, None] * pair_out.astype(jnp.float32), axis=1)
    shared_out = swiglu(x_norm, ws_gate, ws_up, ws_down)
    return (x_f32 + shared_out.astype(jnp.float32) + routed).astype(jnp.bfloat16)
```

```python
import functools

import jax
import jax.numpy as jnp
from jax import lax
from jax.experimental import pallas as pl
from jax.experimental.pallas import tpu as pltpu
from jax.sharding import PartitionSpec as P

NORM_EPS = 1e-6
ROUTE_SCALE = 2.5
GROUPS = 8
GROUP_LIMIT = 4
F32 = jnp.float32
BF16 = jnp.bfloat16
VMEM_LIMIT = 67_000_000


def dot_f32(a, b):
    return jnp.dot(a, b, preferred_element_type=F32)


def place():
    me = lax.axis_index("ep")
    core = lax.rem(me, 2)
    x = lax.rem(me // 2, 2)
    y = me // 4
    return me, core, x, y, me + 1 - 2 * core, me + 2 - 4 * x, me + 4 - 8 * y


def pos_of(dev):
    return lax.rem(dev, 2) * 4 + dev // 2


def rcopy(src, dst, ssem, rsem, dev):
    return pltpu.make_async_remote_copy(
        src_ref=src, dst_ref=dst, send_sem=ssem, recv_sem=rsem, device_id={"ep": dev}, device_id_type=pl.DeviceIdType.MESH
    )


def gather_up_kernel(
    n_kc, cap, hid_ref, gain_ref, rw_ref, ids_ref, wg_ref, wu_ref, h_ref, rg_ref, xn_ref,
    xall, onehot, acc, wbuf, hbuf, xe, rank_s, meta_s, meta_r, w_sem, h_sem, m_send, m_recv, a_send, a_recv,
):
    me, core, x, y, sib, xnb, ynb = place()
    tok, dim = hid_ref.shape
    n_exp, _, inter = wg_ref.shape
    kw = dim // n_kc
    half = tok // 2
    grp = acc.shape[0]
    n_steps = n_exp * n_kc
    slots = wbuf.shape[0]

    def step_of(s):
        g = s // (grp * n_kc)
        r = lax.rem(s, grp * n_kc)
        return g * grp + lax.rem(r, grp), lax.rem(r, grp), r // grp

    def w_copies(s):
        e, _, kc = step_of(s)
        slot = lax.rem(s, slots)
        rows = pl.ds(pl.multiple_of(kc * kw, kw), kw)
        return (
            pltpu.make_async_copy(wg_ref.at[e, rows, :], wbuf.at[slot, :, pl.ds(0, inter)], w_sem.at[slot, 0]),
            pltpu.make_async_copy(wu_ref.at[e, rows, :], wbuf.at[slot, :, pl.ds(inter, inter)], w_sem.at[slot, 1]),
        )

    def w_start(s):
        for c in w_copies(s):
            c.start()

    for s in range(slots - 1):
        w_start(jnp.int32(s))

    barrier = pltpu.get_barrier_semaphore()
    for k in range(1, 8):
        pl.semaphore_signal(barrier, inc=1, device_id={"ep": lax.rem(me + k, 8)}, device_id_type=pl.DeviceIdType.MESH)

    x_f32 = hid_ref[...].astype(F32)
    inv_rms = lax.rsqrt(jnp.mean(x_f32 * x_f32, axis=-1, keepdims=True) + NORM_EPS)
    x_norm = (x_f32 * inv_rms * gain_ref[...]).astype(BF16)
    xn_ref[...] = x_norm
    my_pos = pos_of(me)
    my_rows = pl.ds(pl.multiple_of(my_pos * tok, tok), tok)
    for kc in range(n_kc):
        xall[kc, my_rows, :] = x_norm[:, kc * kw : (kc + 1) * kw]

    pl.semaphore_wait(barrier, 7)

    def block(kc, dev, part=None):
        start = pos_of(dev) * tok + (0 if part is None else part * half)
        n = tok if part is None else half
        return xall.at[kc, pl.ds(pl.multiple_of(start, half), n), :]

    def send(kc, kind, dev_src, to, part=None):
        ref = block(kc, dev_src, part)
        return rcopy(ref, ref, a_send.at[kc, kind], a_recv.at[kc, kind], to)

    diag = me + 6 - 4 * x - 8 * y
    kinds = (
        (me, sib, None), (me, xnb, None), (me, ynb, None), (xnb, ynb, 0), (ynb, xnb, 1),
        (xnb, sib, None), (ynb, sib, None), (diag, sib, 0), (diag, sib, 1),
    )

    def copy(kc, kind):
        src, to, part = kinds[kind]
        return send(kc, kind, src, to, part)

    def start(kc, which):
        for kind in which:
            copy(kc, kind).start()

    def received(kc, which):
        for kind in which:
            copy(kc, kind).wait_recv()

    def serve_a(kc):
        received(kc, (1, 2))
        start(kc, (3, 4, 5, 6))
        if kc + 1 < n_kc:
            start(kc + 1, (1, 2, 0))

    def serve_b(kc):
        received(kc, (3, 4))
        start(kc, (7, 8))

    def arrived(kc):
        received(kc, (0, 5, 6, 7, 8))

    start(0, (1, 2, 0))

    logits = lax.dot_general(
        rw_ref[...], x_norm.astype(F32), (((1,), (1,)), ((), ())), precision=lax.Precision.HIGHEST, preferred_element_type=F32
    )
    scores = jax.nn.sigmoid(logits)
    exp_iota = lax.broadcasted_iota(jnp.int32, scores.shape, 0)
    chosen = exp_iota == ids_ref[0:1, :tok]
    for j in range(1, 6):
        chosen = chosen | (exp_iota == ids_ref[j : j + 1, :tok])
    picked = jnp.where(chosen, scores, 0.0)
    gates = ROUTE_SCALE * picked / jnp.sum(picked, axis=0, keepdims=True)
    gates = jnp.where(chosen, gates, -1.0)
    meta_s[...] = jnp.full(meta_s.shape, -1.0, F32)
    for d in range(8):
        meta_s[d, :, 0:tok] = gates[d * n_exp : (d + 1) * n_exp, :]
    meta_r[pl.ds(my_pos, 1)] = meta_s[pl.ds(me, 1)]

    def meta(k):
        to = lax.rem(me + k, 8)
        return rcopy(meta_s.at[to], meta_r.at[my_pos], m_send.at[k], m_recv.at[k], to)

    for k in range(1, 8):
        meta(k).start()
    for k in range(1, 8):
        meta(k).wait_recv()

    lane = lax.broadcasted_iota(jnp.int32, (n_exp, 128), 1)
    tiles = []
    for m in range(4):
        a = meta_r[2 * m]
        b = pltpu.roll(meta_r[2 * m + 1], 64, 1)
        tiles += [a[:, :128], jnp.where(lane < 64, a[:, 128:], b[:, :128]), b[:, 128:]]
    masks = [t >= 0.0 for t in tiles]
    ones = jnp.concatenate([jnp.where(m, 1.0, 0.0) for m in masks], axis=0).astype(BF16)
    upper = lax.broadcasted_iota(jnp.int32, (128, 128), 0) <= lax.broadcasted_iota(jnp.int32, (128, 128), 1)
    counts = dot_f32(ones, jnp.where(upper, 1.0, 0.0).astype(BF16))
    before = jnp.zeros((n_exp, 1), F32)
    for i in range(12):
        cum = counts[i * n_exp : (i + 1) * n_exp]
        rank = jnp.where(masks[i], cum - 1.0 + before, -1.0)
        before = before + cum[:, 127:128]
        gate = jnp.where(masks[i], tiles[i], 0.0)
        for e in range(n_exp):
            rank_s[e, :, i * 128 : (i + 1) * 128] = rank[e : e + 1]
        packed = jnp.concatenate([rank, gate, jnp.zeros((128 - 2 * n_exp, 128), F32)], axis=0)
        rg_ref[i * 128 : (i + 1) * 128, :] = packed.T

    slot_iota = lax.broadcasted_iota(jnp.int32, (cap, 128), 0).astype(F32)

    def build(e, carry):
        for i in range(12):
            row = rank_s[e, :, i * 128 : (i + 1) * 128]
            onehot[e, :, i * 128 : (i + 1) * 128] = jnp.where(row == slot_iota, 1.0, 0.0).astype(BF16)
        return carry

    lax.fori_loop(0, n_exp, build, 0)

    serve_a(0)
    serve_b(0)
    arrived(0)

    def step(s, carry):
        e, el, kc = step_of(s)
        for c in range(1, n_kc):
            pl.when(s == grp * (c - 1) + 1)(functools.partial(serve_a, c))
            pl.when(s == grp * (c - 1) + grp - 1)(functools.partial(serve_b, c))
            pl.when(s == grp * c)(functools.partial(arrived, c))

        @pl.when(s + slots - 1 < n_steps)
        def _():
            w_start(s + slots - 1)

        for n in range(0, kw, 256):
            xe[:, n : n + 256] = dot_f32(onehot[e], xall[kc, :, n : n + 256]).astype(BF16)
        for c in w_copies(s):
            c.wait()
        slot = lax.rem(s, slots)
        for n in range(0, 2 * inter, 256):
            part = dot_f32(xe[...], wbuf[slot, :, n : n + 256])
            acc[el, :, n : n + 256] = jnp.where(kc > 0, acc[el, :, n : n + 256], 0.0) + part

        @pl.when(kc == n_kc - 1)
        def _():
            for n in range(0, inter, 128):
                g = acc[el, :, n : n + 128]
                u = acc[el, :, inter + n : inter + n + 128]
                hbuf[e, :, n : n + 128] = (jax.nn.silu(g) * u).astype(BF16)
            pltpu.make_async_copy(hbuf.at[e], h_ref.at[e], h_sem.at[e]).start()

        return carry

    lax.fori_loop(0, n_steps, step, 0)

    for e in range(n_exp):
        pltpu.make_async_copy(hbuf.at[e], h_ref.at[e], h_sem.at[e]).wait()
    for k in range(1, 8):
        meta(k).wait_send()
    for kc in range(n_kc):
        for kind in range(len(kinds)):
            copy(kc, kind).wait_send()


def down_kernel(
    n_chunk, hid_ref, xn_ref, rg_ref, h_ref, wd_ref, wsg_ref, wsu_ref, wsd_ref, out_ref,
    hv, place_t, gcol, wdb, part, got0, mid, got1, quart, got2, total, wsb, wdsb, hs,
    hv_sem, wd_sem, ws_sem, wds_sem, d_send, d_recv, p_send, p_recv, q_send, q_recv,
):
    me, core, x, y, sib, xnb, ynb = place()
    n_exp, cap, inter = h_ref.shape
    tok, dim = hid_ref.shape
    ctok = 4 * tok
    cw = dim // n_chunk
    hw = cw // 2
    unroll = 2
    per_chunk = n_exp // unroll
    n_steps = n_chunk * per_chunk
    slots = wdb.shape[0]

    def wd_copy(i):
        e, n, slot = lax.rem(i, n_exp), i // n_exp, lax.rem(i, slots)
        return pltpu.make_async_copy(wd_ref.at[e, :, pl.ds(pl.multiple_of(n * cw, cw), cw)], wdb.at[slot], wd_sem.at[slot])

    def h_copy(e):
        return pltpu.make_async_copy(h_ref.at[e], hv.at[e], hv_sem.at[e])

    h_copy(0).start()
    for i in range(slots - unroll):
        wd_copy(jnp.int32(i)).start()
    for e in range(1, n_exp):
        h_copy(e).start()

    barrier = pltpu.get_barrier_semaphore()
    for dev in (sib, xnb, ynb):
        pl.semaphore_signal(barrier, inc=1, device_id={"ep": dev}, device_id_type=pl.DeviceIdType.MESH)

    slot_iota = lax.broadcasted_iota(jnp.int32, (8 * tok, cap), 1).astype(F32)
    for e in range(n_exp):
        place_t[e] = jnp.where(rg_ref[:, e : e + 1] == slot_iota, 1.0, 0.0).astype(BF16)
        gcol[e] = jnp.broadcast_to(rg_ref[:, n_exp + e : n_exp + e + 1], (8 * tok, hw))
    pl.semaphore_wait(barrier, 3)

    def d_copy(n):
        b = lax.rem(n, 2)
        return rcopy(part.at[b, :, 1 - core], got0.at[b], d_send.at[b], d_recv.at[b], sib)

    def p_copies(n):
        b = lax.rem(n, 2)
        return (
            rcopy(mid.at[b, 0, :, 1 - x], got1.at[b, 0], p_send.at[b, 0], p_recv.at[b, 0], xnb),
            rcopy(mid.at[b, 1, 1 - y], got1.at[b, 1], p_send.at[b, 1], p_recv.at[b, 1], ynb),
        )

    def q_copies(n):
        b = lax.rem(n, 2)
        return (
            rcopy(quart.at[b, 0, 1 - y], got2.at[b, 0], q_send.at[b, 0], q_recv.at[b, 0], ynb),
            rcopy(quart.at[b, 1, 1 - x], got2.at[b, 1], q_send.at[b, 1], q_recv.at[b, 1], xnb),
        )

    def start(copies):
        for c in copies:
            c.start()

    def wait(copies):
        for c in copies:
            c.wait()

    def stage_p(n):
        b = lax.rem(n, 2)
        d_copy(n).wait()
        for hf in range(2):
            for yy in range(2):
                for xx in range(2):
                    rows = pl.ds((yy * 2 + xx) * tok, tok)
                    mid[b, hf, yy, xx] = part[b, hf, core, rows, :] + got0[b, hf, rows, :]
        start(p_copies(n))

    def stage_q(n):
        b = lax.rem(n, 2)
        wait(p_copies(n))
        for k in range(2):
            quart[b, 0, k] = mid[b, 0, k, x] + got1[b, 0, k]
            quart[b, 1, k] = mid[b, 1, y, k] + got1[b, 1, k]
        start(q_copies(n))

    def stage_f(n):
        b = lax.rem(n, 2)
        wait(q_copies(n))
        total[n, 0] = quart[b, 0, y] + got2[b, 0]
        total[n, 1] = quart[b, 1, x] + got2[b, 1]

    def step(s, carry):
        n, j = s // per_chunk, lax.rem(s, per_chunk)
        b = lax.rem(n, 2)

        for u in range(unroll):
            i = s * unroll + slots - unroll + u

            @pl.when(i < n_chunk * n_exp)
            def _():
                wd_copy(i).start()

        @pl.when(n == 0)
        def _():
            for u in range(unroll):
                h_copy(j * unroll + u).wait()

        for u in range(unroll):
            wd_copy(s * unroll + u).wait()

        outs = []
        for u in range(unroll):
            e = j * unroll + u
            slot = lax.rem(s * unroll + u, slots)
            outs.append(dot_f32(hv[e], wdb[slot]).astype(BF16))
        for half in range(2):
            rows = pl.ds(half * ctok, ctok)
            new = [dot_f32(place_t[j * unroll + u, rows, :], outs[u]) for u in range(unroll)]
            for hf in range(2):
                cols = slice(hf * hw, (hf + 1) * hw)
                val = jnp.where(j > 0, part[b, hf, half], 0.0)
                for u in range(unroll):
                    val = val + gcol[j * unroll + u, rows, :] * new[u][:, cols]
                part[b, hf, half] = val

        @pl.when(j == per_chunk // 2 - 1)
        def _():
            pl.when(n >= 3)(lambda: stage_f(n - 3))
            pl.when(n >= 2)(lambda: stage_q(n - 2))
            pl.when(n >= 1)(lambda: stage_p(n - 1))

        pl.when(j == per_chunk - 1)(lambda: d_copy(n).start())
        return carry

    lax.fori_loop(0, n_steps, step, 0)

    sw = wsb.shape[-1] // 2
    n_s = wsg_ref.shape[1] // sw

    def ws_copies(i):
        cols = pl.ds(pl.multiple_of(i * sw, sw), sw)
        slot = lax.rem(i, 2)
        return (
            pltpu.make_async_copy(wsg_ref.at[:, cols], wsb.at[slot, :, pl.ds(0, sw)], ws_sem.at[slot, 0]),
            pltpu.make_async_copy(wsu_ref.at[:, cols], wsb.at[slot, :, pl.ds(sw, sw)], ws_sem.at[slot, 1]),
        )

    last = jnp.int32(n_chunk - 1)
    start(ws_copies(jnp.int32(0)))
    stage_f(last - 2)
    stage_q(last - 1)
    stage_p(last)

    def shared_up(i, carry):
        @pl.when(i + 1 < n_s)
        def _():
            start(ws_copies(i + 1))

        wait(ws_copies(i))
        both = dot_f32(xn_ref[...], wsb[lax.rem(i, 2)])
        hs[i] = (jax.nn.silu(both[:, :sw]) * both[:, sw:]).astype(BF16)

        @pl.when(i == n_s // 2)
        def _():
            stage_f(last - 1)
            stage_q(last)

        return carry

    lax.fori_loop(0, n_s, shared_up, 0)

    dw = wdsb.shape[-1]
    n_d = dim // dw

    def wds_copy(i):
        slot = lax.rem(i, 2)
        return pltpu.make_async_copy(wsd_ref.at[:, pl.ds(pl.multiple_of(i * dw, dw), dw)], wdsb.at[slot], wds_sem.at[slot])

    wds_copy(jnp.int32(0)).start()
    stage_f(last)
    for i in range(n_d):
        if i + 1 < n_d:
            wds_copy(jnp.int32(i + 1)).start()
        wds_copy(jnp.int32(i)).wait()
        res = jnp.zeros((tok, dw), F32)
        for k in range(n_s):
            res = res + dot_f32(hs[k], wdsb[i % 2, k * sw : (k + 1) * sw, :])
        shared = res.astype(BF16).astype(F32)
        for c in range(0, dw, hw):
            col = i * dw + c
            routed = total[col // cw, (col % cw) // hw]
            cols = slice(col, col + hw)
            out_ref[:, cols] = (hid_ref[:, cols].astype(F32) + shared[:, c : c + hw] + routed).astype(BF16)


def solution(mesh):
    ep_size = mesh.shape["ep"]
    assert ep_size == 8

    def local_block(hidden_in, norm_gain, router_w, w_gate, w_up, w_down, ws_gate, ws_up, ws_down, expert_ids):
        tok, top_k = expert_ids.shape
        dim = hidden_in.shape[1]
        n_exp, _, inter = w_gate.shape
        s_inter = ws_gate.shape[1]
        cap = GROUPS * ((top_k + GROUP_LIMIT - 1) // GROUP_LIMIT) * tok // n_exp
        n_kc, grp, slots = 4, 4, 3
        vmem = pl.BlockSpec(memory_space=pltpu.VMEM)
        hbm = pl.BlockSpec(memory_space=pl.ANY)
        dma = pltpu.SemaphoreType.DMA
        ids_t = jnp.pad(expert_ids.T, ((0, 8 - top_k), (0, 256 - tok)), constant_values=-1)

        h, rg, xn = pl.pallas_call(
            functools.partial(gather_up_kernel, n_kc, cap),
            out_shape=(
                jax.ShapeDtypeStruct((n_exp, cap, inter), BF16),
                jax.ShapeDtypeStruct((8 * tok, 128), F32),
                jax.ShapeDtypeStruct((tok, dim), BF16),
            ),
            in_specs=[vmem, vmem, vmem, vmem, hbm, hbm],
            out_specs=(hbm, vmem, vmem),
            scratch_shapes=[
                pltpu.VMEM((n_kc, 8 * tok, dim // n_kc), BF16),
                pltpu.VMEM((n_exp, cap, 8 * tok), BF16),
                pltpu.VMEM((grp, cap, 2 * inter), F32),
                pltpu.VMEM((slots, dim // n_kc, 2 * inter), BF16),
                pltpu.VMEM((n_exp, cap, inter), BF16),
                pltpu.VMEM((cap, dim // n_kc), BF16),
                pltpu.VMEM((n_exp, 1, 8 * tok), F32),
                pltpu.VMEM((8, n_exp, 256), F32),
                pltpu.VMEM((8, n_exp, 256), F32),
                dma((slots, 2)),
                dma((n_exp,)),
                dma((8,)),
                dma((8,)),
                dma((n_kc, 9)),
                dma((n_kc, 9)),
            ],
            compiler_params=pltpu.CompilerParams(collective_id=0, has_side_effects=True, vmem_limit_bytes=VMEM_LIMIT),
            name="gather_up",
        )(hidden_in, norm_gain.reshape(1, dim), router_w, ids_t, w_gate, w_up)

        n_chunk, dslots = 8, 6
        cw = dim // n_chunk
        hw = cw // 2
        sw, dw = 256, 512
        return pl.pallas_call(
            functools.partial(down_kernel, n_chunk),
            out_shape=jax.ShapeDtypeStruct((tok, dim), BF16),
            in_specs=[vmem, vmem, vmem, hbm, hbm, hbm, hbm, hbm],
            out_specs=vmem,
            scratch_shapes=[
                pltpu.VMEM((n_exp, cap, inter), BF16),
                pltpu.VMEM((n_exp, 8 * tok, cap), BF16),
                pltpu.VMEM((n_exp, 8 * tok, hw), F32),
                pltpu.VMEM((dslots, inter, cw), BF16),
                pltpu.VMEM((2, 2, 2, 4 * tok, hw), F32),
                pltpu.VMEM((2, 2, 4 * tok, hw), F32),
                pltpu.VMEM((2, 2, 2, 2, tok, hw), F32),
                pltpu.VMEM((2, 2, 2, tok, hw), F32),
                pltpu.VMEM((2, 2, 2, tok, hw), F32),
                pltpu.VMEM((2, 2, tok, hw), F32),
                pltpu.VMEM((n_chunk, 2, tok, hw), F32),
                pltpu.VMEM((2, dim, 2 * sw), BF16),
                pltpu.VMEM((2, s_inter, dw), BF16),
                pltpu.VMEM((s_inter // sw, tok, sw), BF16),
                dma((n_exp,)),
                dma((dslots,)),
                dma((2, 2)),
                dma((2,)),
                dma((2,)),
                dma((2,)),
                dma((2, 2)),
                dma((2, 2)),
                dma((2, 2)),
                dma((2, 2)),
            ],
            compiler_params=pltpu.CompilerParams(collective_id=1, has_side_effects=True, vmem_limit_bytes=VMEM_LIMIT),
            name="down_sum",
        )(hidden_in, xn, rg, h, w_down, ws_gate, ws_up, ws_down)

    row_spec = P(("dp", "ep"), None)
    in_specs = (row_spec, P(), P(), P("ep"), P("ep"), P("ep"), P(), P(), P(), row_spec)
    return jax.shard_map(local_block, mesh=mesh, in_specs=in_specs, out_specs=row_spec, check_vma=False)
```

```python
import functools

import jax
import jax.numpy as jnp
from jax import lax
from jax.experimental import pallas as pl
from jax.experimental.pallas import tpu as pltpu
from jax.sharding import PartitionSpec as P

NORM_EPS = 1e-6
ROUTE_SCALE = 2.5
GROUPS = 8
GROUP_LIMIT = 4
F32 = jnp.float32
BF16 = jnp.bfloat16
VMEM_LIMIT = 67_000_000
TILE = 16


def dot_f32(a, b):
    return jnp.dot(a, b, preferred_element_type=F32)


def place():
    me = lax.axis_index("ep")
    core = lax.rem(me, 2)
    x = lax.rem(me // 2, 2)
    y = me // 4
    return me, core, x, y, me + 1 - 2 * core, me + 2 - 4 * x, me + 4 - 8 * y


def pos_of(dev):
    return lax.rem(dev, 2) * 4 + dev // 2


def rcopy(src, dst, ssem, rsem, dev):
    return pltpu.make_async_remote_copy(
        src_ref=src, dst_ref=dst, send_sem=ssem, recv_sem=rsem, device_id={"ep": dev}, device_id_type=pl.DeviceIdType.MESH
    )


def split3(v):
    hi = v.astype(BF16)
    rest = v - hi.astype(F32)
    mid = rest.astype(BF16)
    return hi, mid, (rest - mid.astype(F32)).astype(BF16)


def iota(shape, axis):
    return lax.broadcasted_iota(jnp.int32, shape, axis)


def gather_up_kernel(
    n_kc, hid_ref, gain_ref, rw_ref, ids_ref, wg_ref, wu_ref, h_ref, rg_ref, xn_ref, tab_ref, back_ref,
    xall, pick, xsrc, acc, wbuf, hbuf, xe, meta_s, meta_r, ids_r, tab_v, tab_s,
    w_sem, h_sem, t_sem, i_send, i_recv, m_send, m_recv, a_send, a_recv,
):
    me, core, x, y, sib, xnb, ynb = place()
    tok, dim = hid_ref.shape
    n_exp, _, inter = wg_ref.shape
    cap = h_ref.shape[1]
    kw = dim // n_kc
    half = tok // 2
    n_steps = n_exp * n_kc
    slots = wbuf.shape[0]
    n_et = cap // TILE
    n_st = pick.shape[1] // TILE

    def w_copies(s):
        e, kc, slot = lax.rem(s, n_exp), s // n_exp, lax.rem(s, slots)
        rows = pl.ds(pl.multiple_of(kc * kw, kw), kw)
        return (
            pltpu.make_async_copy(wg_ref.at[e, rows, :], wbuf.at[slot, :, pl.ds(0, inter)], w_sem.at[slot, 0]),
            pltpu.make_async_copy(wu_ref.at[e, rows, :], wbuf.at[slot, :, pl.ds(inter, inter)], w_sem.at[slot, 1]),
        )

    def w_start(s):
        for c in w_copies(s):
            c.start()

    for s in range(slots - 1):
        w_start(jnp.int32(s))

    barrier = pltpu.get_barrier_semaphore()
    for k in range(1, 8):
        pl.semaphore_signal(barrier, inc=1, device_id={"ep": lax.rem(me + k, 8)}, device_id_type=pl.DeviceIdType.MESH)

    x_f32 = hid_ref[...].astype(F32)
    inv_rms = lax.rsqrt(jnp.mean(x_f32 * x_f32, axis=-1, keepdims=True) + NORM_EPS)
    x_norm = (x_f32 * inv_rms * gain_ref[...]).astype(BF16)
    xn_ref[...] = x_norm
    my_pos = pos_of(me)
    my_rows = pl.ds(pl.multiple_of(my_pos * tok, tok), tok)
    for kc in range(n_kc):
        xall[kc, my_rows, :] = x_norm[:, kc * kw : (kc + 1) * kw]

    pl.semaphore_wait(barrier, 7)

    def block(kc, dev, part=None):
        start = pos_of(dev) * tok + (0 if part is None else part * half)
        n = tok if part is None else half
        return xall.at[kc, pl.ds(pl.multiple_of(start, half), n), :]

    def send(kc, kind, dev_src, to, part=None):
        ref = block(kc, dev_src, part)
        return rcopy(ref, ref, a_send.at[kc, kind], a_recv.at[kc, kind], to)

    diag = me + 6 - 4 * x - 8 * y
    kinds = (
        (me, sib, None), (me, xnb, None), (me, ynb, None), (xnb, ynb, 0), (ynb, xnb, 1),
        (xnb, sib, None), (ynb, sib, None), (diag, sib, 0), (diag, sib, 1),
    )

    def copy(kc, kind):
        src, to, part = kinds[kind]
        return send(kc, kind, src, to, part)

    def start(kc, which):
        for kind in which:
            copy(kc, kind).start()

    def received(kc, which):
        for kind in which:
            copy(kc, kind).wait_recv()

    def serve_a(kc):
        received(kc, (1, 2))
        start(kc, (3, 4, 5, 6))
        if kc + 1 < n_kc:
            start(kc + 1, (1, 2, 0))

    def serve_b(kc):
        received(kc, (3, 4))
        start(kc, (7, 8))

    def meta(k):
        to = lax.rem(me + k, 8)
        return rcopy(meta_s.at[to], meta_r.at[my_pos], m_send.at[k], m_recv.at[k], to)

    def ids_copy(k):
        return rcopy(ids_ref, ids_r.at[my_pos], i_send.at[k], i_recv.at[k], lax.rem(me + k, 8))

    for k in range(1, 8):
        ids_copy(k).start()
    start(0, (1, 2, 0))
    ids_r[pl.ds(my_pos, 1)] = ids_ref[...].reshape(1, 8, 256)

    parts = lax.dot_general(
        jnp.concatenate(split3(rw_ref[...]), axis=0), x_norm, (((1,), (1,)), ((), ())), preferred_element_type=F32
    )
    logits = parts[:64] + (parts[64:128] + parts[128:192])
    scores = jax.nn.sigmoid(logits)
    exp_iota = iota(scores.shape, 0)
    chosen = exp_iota == ids_ref[0:1, :tok]
    for j in range(1, 6):
        chosen = chosen | (exp_iota == ids_ref[j : j + 1, :tok])
    picked = jnp.where(chosen, scores, 0.0)
    gates = ROUTE_SCALE * picked / jnp.sum(picked, axis=0, keepdims=True)
    meta_s[...] = jnp.zeros(meta_s.shape, F32)
    for d in range(8):
        meta_s[d, :, 0:tok] = gates[d * n_exp : (d + 1) * n_exp, :]
    meta_r[pl.ds(my_pos, 1)] = meta_s[pl.ds(me, 1)]
    for k in range(1, 8):
        meta(k).start()
    for k in range(1, 8):
        ids_copy(k).wait_recv()

    my_exp = me * n_exp + iota((n_exp, 256), 0)
    masks = []
    for s in range(8):
        hit = my_exp == ids_r[s, 0:1, :]
        for j in range(1, 6):
            hit = hit | (my_exp == ids_r[s, j : j + 1, :])
        masks.append(hit)
    ones = jnp.concatenate([jnp.where(m, 1.0, 0.0) for m in masks], axis=0).astype(BF16)
    upper = iota((256, 256), 0) <= iota((256, 256), 1)
    cums = dot_f32(ones, jnp.where(upper, 1.0, 0.0).astype(BF16))
    cums = [cums[s * n_exp : (s + 1) * n_exp] for s in range(8)]

    lane = iota((n_exp, 128), 1)
    base = jnp.zeros((n_exp, 128), F32)
    count = jnp.zeros((n_exp, 128), F32)
    before = jnp.zeros((n_exp, 1), F32)
    for s in range(8):
        n = cums[s][:, 255:256]
        base = jnp.where(lane == s, before, base)
        count = jnp.where(lane == s, n, count)
        before = before + n
    base, count = base.astype(jnp.int32), count.astype(jnp.int32)
    first = base // TILE
    tiles = jnp.where(count > 0, (base + count - 1) // TILE - first + 1, 0)
    sub = iota((n_exp, 128), 0)
    ends = tiles
    for d in (1, 2, 4):
        ends = ends + jnp.where(sub >= d, pltpu.roll(ends, d, 0), 0)
    begin = ends - tiles
    shift = ((begin - first) * TILE + base).astype(F32)

    slot_ids = []
    for s in range(8):
        slot_ids.append(jnp.where(masks[s], cums[s] - 1.0 + shift[:, s : s + 1], -1.0))

    def build(s, ids):
        for q in range(0, n_st * TILE, 128):
            want = (iota((128, 256), 0) + q).astype(F32)
            got = want == ids[0:1]
            for e in range(1, n_exp):
                got = got | (want == ids[e : e + 1])
            pick[s, q : q + 128, :] = jnp.where(got, 1.0, 0.0).astype(BF16)[:, :tok]

    for s in range(8):
        build(s, slot_ids[s])

    rows24 = jnp.concatenate([first, tiles, begin], axis=0).astype(F32).astype(BF16)
    src = iota((128, 768), 0)
    col = iota((128, 768), 1)
    spread = jnp.where(jnp.where(col < 256, col % 8, (col - 256) // 64) == src, 1.0, 0.0).astype(BF16)
    table = dot_f32(rows24, spread).astype(jnp.int32)
    t_first, t_tiles, t_begin = table[:n_exp], table[n_exp : 2 * n_exp], table[2 * n_exp :]
    col = iota((n_exp, 256), 1)
    nth = col // 8 - t_first[:, :256]
    valid = (nth >= 0) & (nth < t_tiles[:, :256])
    tab_v[...] = jnp.where(valid, (col % 8) * n_st + t_begin[:, :256] + nth, 8 * n_st)
    out = pltpu.make_async_copy(tab_v, tab_ref, t_sem.at[0])
    out.start()
    nth = iota((n_exp, 512), 1) % 64 - t_begin[:, 256:]
    valid = (nth >= 0) & (nth < t_tiles[:, 256:])
    back = jnp.where(valid, iota((n_exp, 512), 0) * n_et + t_first[:, 256:] + nth, 0)
    back_ref[...] = jnp.sum(back, axis=0, keepdims=True)
    out.wait()
    load = pltpu.make_async_copy(tab_ref, tab_s, t_sem.at[1])
    load.start()

    serve_a(0)

    for k in range(1, 8):
        meta(k).wait_recv()
    for s in range(8):
        packed = jnp.concatenate([slot_ids[s], meta_r[s], jnp.zeros((128 - 2 * n_exp, 256), F32)], axis=0)
        rg_ref[s] = packed.T[:tok]
    xsrc[8 * n_st] = jnp.zeros((TILE, kw), BF16)
    load.wait()

    def select(kc):
        received(kc, (0, 5, 6, 7, 8))

        def one(s, carry):
            rows = xall[kc, pl.ds(pl.multiple_of(s * tok, tok), tok), :]
            res = dot_f32(pick[s], rows).astype(BF16)
            xsrc[pl.ds(s * n_st, n_st)] = res.reshape(n_st, TILE, kw)
            return carry

        lax.fori_loop(0, 8, one, 0)

    def fill(s):
        e, slot = lax.rem(s, n_exp), lax.rem(s, 2)
        for t in range(n_et):
            got = [xsrc[jnp.clip(tab_s[e, t * 8 + k], 0, 8 * n_st)] for k in range(8)]
            while len(got) > 1:
                got = [got[i] + got[i + 1] for i in range(0, len(got), 2)]
            xe[slot, t * TILE : (t + 1) * TILE, :] = got[0]

    serve_b(0)
    select(0)
    fill(jnp.int32(0))

    def step(s, carry):
        e, kc = lax.rem(s, n_exp), s // n_exp
        slot = lax.rem(s, slots)
        for c in range(1, n_kc):
            pl.when(s == n_exp * (c - 1) + 2)(functools.partial(serve_a, c))
            pl.when(s == n_exp * (c - 1) + 5)(functools.partial(serve_b, c))
            pl.when(s == n_exp * c - 1)(functools.partial(select, c))

        @pl.when(s + slots - 1 < n_steps)
        def _():
            w_start(s + slots - 1)

        for c in w_copies(s):
            c.wait()
        fill(s + 1)
        for n in range(0, 2 * inter, 256):
            part = dot_f32(xe[lax.rem(s, 2)], wbuf[slot, :, n : n + 256])
            acc[e, :, n : n + 256] = jnp.where(kc > 0, acc[e, :, n : n + 256], 0.0) + part

        @pl.when(kc == n_kc - 1)
        def _():
            b = lax.rem(e, 2)

            @pl.when(e >= 2)
            def _():
                pltpu.make_async_copy(hbuf.at[b], h_ref.at[e - 2], h_sem.at[b]).wait()

            for n in range(0, inter, 128):
                g = acc[e, :, n : n + 128]
                u = acc[e, :, inter + n : inter + n + 128]
                hbuf[b, :, n : n + 128] = (jax.nn.silu(g) * u).astype(BF16)
            pltpu.make_async_copy(hbuf.at[b], h_ref.at[e], h_sem.at[b]).start()

        return carry

    lax.fori_loop(0, n_steps, step, 0)

    for e in range(n_exp - 2, n_exp):
        pltpu.make_async_copy(hbuf.at[e % 2], h_ref.at[e], h_sem.at[e % 2]).wait()
    for k in range(1, 8):
        ids_copy(k).wait_send()
        meta(k).wait_send()
    for kc in range(n_kc):
        for kind in range(len(kinds)):
            copy(kc, kind).wait_send()


def down_kernel(
    n_chunk, hid_ref, xn_ref, rg_ref, back_ref, h_ref, wd_ref, wsg_ref, wsu_ref, wsd_ref, out_ref,
    hv, weigh, wdb, etile, esrc, part, got0, mid, got1, quart, got2, total, wsb, wdsb, hs,
    hv_sem, wd_sem, ws_sem, wds_sem, d_send, d_recv, p_send, p_recv, q_send, q_recv,
):
    me, core, x, y, sib, xnb, ynb = place()
    n_exp, cap, inter = h_ref.shape
    tok, dim = hid_ref.shape
    n_et = cap // TILE
    n_slot = weigh.shape[-1]
    n_st = n_slot // TILE
    cw = dim // n_chunk
    hw = cw // 2
    unroll = 2
    n_down = n_exp // unroll
    per_src = 4
    per_chunk = n_down + 8 // per_src + 2
    n_steps = n_chunk * per_chunk
    slots = wdb.shape[0]
    sw = wsb.shape[-1] // 2
    n_s = wsg_ref.shape[1] // sw
    dw = wdsb.shape[-1]
    n_d = dim // dw

    def wd_copy(i):
        e, n, slot = lax.rem(i, n_exp), i // n_exp, lax.rem(i, slots)
        return pltpu.make_async_copy(wd_ref.at[e, :, pl.ds(pl.multiple_of(n * cw, cw), cw)], wdb.at[slot], wd_sem.at[slot])

    def h_copy(e):
        return pltpu.make_async_copy(h_ref.at[e], hv.at[e], hv_sem.at[e])

    def ws_copies(i):
        cols = pl.ds(pl.multiple_of(i * sw, sw), sw)
        slot = lax.rem(i, 2)
        return (
            pltpu.make_async_copy(wsg_ref.at[:, cols], wsb.at[slot, :, pl.ds(0, sw)], ws_sem.at[slot, 0]),
            pltpu.make_async_copy(wsu_ref.at[:, cols], wsb.at[slot, :, pl.ds(sw, sw)], ws_sem.at[slot, 1]),
        )

    def wds_copy(i):
        slot = lax.rem(i, 2)
        return pltpu.make_async_copy(wsd_ref.at[:, pl.ds(pl.multiple_of(i * dw, dw), dw)], wdsb.at[slot], wds_sem.at[slot])

    def start(copies):
        for c in copies:
            c.start()

    def wait(copies):
        for c in copies:
            c.wait()

    h_copy(0).start()
    for i in range(slots - unroll):
        wd_copy(jnp.int32(i)).start()
    for e in range(1, n_exp):
        h_copy(e).start()
    start(ws_copies(jnp.int32(0)))

    barrier = pltpu.get_barrier_semaphore()
    for dev in (sib, xnb, ynb):
        pl.semaphore_signal(barrier, inc=1, device_id={"ep": dev}, device_id_type=pl.DeviceIdType.MESH)

    def build(s, carry):
        slot = iota((tok, n_slot), 1).astype(F32)
        val = jnp.zeros((tok, n_slot), F32)
        for e in range(n_exp):
            val = jnp.where(rg_ref[s, :, e : e + 1] == slot, rg_ref[s, :, n_exp + e : n_exp + e + 1], val)
        for k, piece in enumerate(split3(val)):
            weigh[s, k * tok : (k + 1) * tok, :] = piece
        return carry

    lax.fori_loop(0, 8, build, 0)
    pl.semaphore_wait(barrier, 3)

    def d_copy(n):
        b = lax.rem(n, 2)
        return rcopy(part.at[b, :, 1 - core], got0.at[b], d_send.at[b], d_recv.at[b], sib)

    def p_copies(n):
        b = lax.rem(n, 2)
        return (
            rcopy(mid.at[b, 0, :, 1 - x], got1.at[b, 0], p_send.at[b, 0], p_recv.at[b, 0], xnb),
            rcopy(mid.at[b, 1, 1 - y], got1.at[b, 1], p_send.at[b, 1], p_recv.at[b, 1], ynb),
        )

    def q_copies(n):
        b = lax.rem(n, 2)
        return (
            rcopy(quart.at[b, 0, 1 - y], got2.at[b, 0], q_send.at[b, 0], q_recv.at[b, 0], ynb),
            rcopy(quart.at[b, 1, 1 - x], got2.at[b, 1], q_send.at[b, 1], q_recv.at[b, 1], xnb),
        )

    def stage_p(n):
        b = lax.rem(n, 2)
        d_copy(n).wait()
        for hf in range(2):
            for yy in range(2):
                for xx in range(2):
                    rows = pl.ds((yy * 2 + xx) * tok, tok)
                    mid[b, hf, yy, xx] = part[b, hf, core, rows, :] + got0[b, hf, rows, :]
        start(p_copies(n))

    def stage_q(n):
        b = lax.rem(n, 2)
        wait(p_copies(n))
        for k in range(2):
            quart[b, 0, k] = mid[b, 0, k, x] + got1[b, 0, k]
            quart[b, 1, k] = mid[b, 1, y, k] + got1[b, 1, k]
        start(q_copies(n))

    def stage_f(n):
        b = lax.rem(n, 2)
        wait(q_copies(n))
        total[n, 0] = quart[b, 0, y] + got2[b, 0]
        total[n, 1] = quart[b, 1, x] + got2[b, 1]

    def down(n, j):
        i0 = n * n_exp + j * unroll
        for u in range(unroll):
            i = i0 + slots - unroll + u

            @pl.when(i < n_chunk * n_exp)
            def _():
                wd_copy(i).start()

        @pl.when(n == 0)
        def _():
            for u in range(unroll):
                h_copy(j * unroll + u).wait()

        for u in range(unroll):
            wd_copy(i0 + u).wait()
        for u in range(unroll):
            e = j * unroll + u
            res = dot_f32(hv[e], wdb[lax.rem(i0 + u, slots)]).astype(BF16)
            etile[pl.ds(e * n_et, n_et)] = res.reshape(n_et, TILE, cw)

    def combine(n, g):
        b = lax.rem(n, 2)
        for u in range(per_src):
            s = g * per_src + u
            for t in range(n_st):
                esrc[u, t * TILE : (t + 1) * TILE, :] = etile[back_ref[0, s * 64 + t]]
        for u in range(per_src):
            s = g * per_src + u
            res = dot_f32(weigh[s], esrc[u])
            res = res[:tok] + (res[tok : 2 * tok] + res[2 * tok :])
            for hf in range(2):
                part[b, hf, s // 4, pl.ds(pl.multiple_of(lax.rem(s, 4) * tok, tok), tok), :] = res[:, hf * hw : (hf + 1) * hw]

    def shared_up(i):
        @pl.when(i + 1 < n_s)
        def _():
            start(ws_copies(i + 1))

        wait(ws_copies(i))
        both = dot_f32(xn_ref[...], wsb[lax.rem(i, 2)])
        hs[i] = (jax.nn.silu(both[:, :sw]) * both[:, sw:]).astype(BF16)

    def step(s, carry):
        n, j = s // per_chunk, lax.rem(s, per_chunk)
        pl.when(j < n_down)(lambda: down(n, j))

        @pl.when((j >= n_down) & (j < per_chunk - 2))
        def _():
            combine(n, j - n_down)

        pl.when(j == per_chunk - 3)(lambda: d_copy(n).start())
        i = n * 2 + j - (per_chunk - 2)
        pl.when((j >= per_chunk - 2) & (i < n_s))(lambda: shared_up(i))

        @pl.when(j == 0)
        def _():
            pl.when(n >= 3)(lambda: stage_f(n - 3))
            pl.when(n >= 2)(lambda: stage_q(n - 2))
            pl.when(n >= 1)(lambda: stage_p(n - 1))

        return carry

    lax.fori_loop(0, n_steps, step, 0)

    last = jnp.int32(n_chunk - 1)
    wds_copy(jnp.int32(0)).start()
    stage_f(last - 2)
    stage_q(last - 1)
    stage_p(last)
    shared = []
    for i in range(n_d):
        if i + 1 < n_d:
            wds_copy(jnp.int32(i + 1)).start()
        wds_copy(jnp.int32(i)).wait()
        res = jnp.zeros((tok, dw), F32)
        for k in range(n_s):
            res = res + dot_f32(hs[k], wdsb[i % 2, k * sw : (k + 1) * sw, :])
        out_ref[:, i * dw : (i + 1) * dw] = res.astype(BF16)
    stage_f(last - 1)
    stage_q(last)
    stage_f(last)
    for n in range(n_chunk):
        for hf in range(2):
            cols = slice(n * cw + hf * hw, n * cw + (hf + 1) * hw)
            out_ref[:, cols] = (hid_ref[:, cols].astype(F32) + out_ref[:, cols].astype(F32) + total[n, hf]).astype(BF16)


def solution(mesh):
    ep_size = mesh.shape["ep"]
    assert ep_size == 8

    def local_block(hidden_in, norm_gain, router_w, w_gate, w_up, w_down, ws_gate, ws_up, ws_down, expert_ids):
        tok, top_k = expert_ids.shape
        dim = hidden_in.shape[1]
        n_exp, _, inter = w_gate.shape
        s_inter = ws_gate.shape[1]
        cap = GROUPS * ((top_k + GROUP_LIMIT - 1) // GROUP_LIMIT) * tok // n_exp
        n_kc, slots = 4, 3
        kw = dim // n_kc
        pair_cap = cap * n_exp // ep_size
        n_st = (pair_cap + 14 * n_exp) // TILE + n_exp
        n_slot = -(-n_st * TILE // 128) * 128
        n_st = n_slot // TILE
        vmem = pl.BlockSpec(memory_space=pltpu.VMEM)
        smem = pl.BlockSpec(memory_space=pltpu.SMEM)
        hbm = pl.BlockSpec(memory_space=pl.ANY)
        dma = pltpu.SemaphoreType.DMA
        ids_t = jnp.pad(expert_ids.T, ((0, 8 - top_k), (0, 256 - tok)), constant_values=-1)

        h, rg, xn, _, back = pl.pallas_call(
            functools.partial(gather_up_kernel, n_kc),
            out_shape=(
                jax.ShapeDtypeStruct((n_exp, cap, inter), BF16),
                jax.ShapeDtypeStruct((8, tok, 128), F32),
                jax.ShapeDtypeStruct((tok, dim), BF16),
                jax.ShapeDtypeStruct((n_exp, 256), jnp.int32),
                jax.ShapeDtypeStruct((1, 512), jnp.int32),
            ),
            in_specs=[vmem, vmem, vmem, vmem, hbm, hbm],
            out_specs=(hbm, vmem, vmem, hbm, vmem),
            scratch_shapes=[
                pltpu.VMEM((n_kc, 8 * tok, kw), BF16),
                pltpu.VMEM((8, n_slot, tok), BF16),
                pltpu.VMEM((8 * n_st + 1, TILE, kw), BF16),
                pltpu.VMEM((n_exp, cap, 2 * inter), F32),
                pltpu.VMEM((slots, kw, 2 * inter), BF16),
                pltpu.VMEM((2, cap, inter), BF16),
                pltpu.VMEM((2, cap, kw), BF16),
                pltpu.VMEM((8, n_exp, 256), F32),
                pltpu.VMEM((8, n_exp, 256), F32),
                pltpu.VMEM((8, 8, 256), jnp.int32),
                pltpu.VMEM((n_exp, 256), jnp.int32),
                pltpu.SMEM((n_exp, 256), jnp.int32),
                dma((slots, 2)),
                dma((2,)),
                dma((2,)),
                dma((8,)),
                dma((8,)),
                dma((8,)),
                dma((8,)),
                dma((n_kc, 9)),
                dma((n_kc, 9)),
            ],
            compiler_params=pltpu.CompilerParams(collective_id=0, has_side_effects=True, vmem_limit_bytes=VMEM_LIMIT),
            name="gather_up",
        )(hidden_in, norm_gain.reshape(1, dim), router_w, ids_t, w_gate, w_up)

        n_chunk, dslots = 8, 6
        cw = dim // n_chunk
        hw = cw // 2
        sw, dw = 256, 512
        return pl.pallas_call(
            functools.partial(down_kernel, n_chunk),
            out_shape=jax.ShapeDtypeStruct((tok, dim), BF16),
            in_specs=[vmem, vmem, vmem, smem, hbm, hbm, hbm, hbm, hbm],
            out_specs=vmem,
            scratch_shapes=[
                pltpu.VMEM((n_exp, cap, inter), BF16),
                pltpu.VMEM((8, 3 * tok, n_slot), BF16),
                pltpu.VMEM((dslots, inter, cw), BF16),
                pltpu.VMEM((n_exp * cap // TILE, TILE, cw), BF16),
                pltpu.VMEM((4, n_slot, cw), BF16),
                pltpu.VMEM((2, 2, 2, 4 * tok, hw), F32),
                pltpu.VMEM((2, 2, 4 * tok, hw), F32),
                pltpu.VMEM((2, 2, 2, 2, tok, hw), F32),
                pltpu.VMEM((2, 2, 2, tok, hw), F32),
                pltpu.VMEM((2, 2, 2, tok, hw), F32),
                pltpu.VMEM((2, 2, tok, hw), F32),
                pltpu.VMEM((n_chunk, 2, tok, hw), F32),
                pltpu.VMEM((2, dim, 2 * sw), BF16),
                pltpu.VMEM((2, s_inter, dw), BF16),
                pltpu.VMEM((s_inter // sw, tok, sw), BF16),
                dma((n_exp,)),
                dma((dslots,)),
                dma((2, 2)),
                dma((2,)),
                dma((2,)),
                dma((2,)),
                dma((2, 2)),
                dma((2, 2)),
                dma((2, 2)),
                dma((2, 2)),
            ],
            compiler_params=pltpu.CompilerParams(collective_id=1, has_side_effects=True, vmem_limit_bytes=VMEM_LIMIT),
            name="down_sum",
        )(hidden_in, xn, rg, back, h, w_down, ws_gate, ws_up, ws_down)

    row_spec = P(("dp", "ep"), None)
    in_specs = (row_spec, P(), P(), P("ep"), P("ep"), P("ep"), P(), P(), P(), row_spec)
    return jax.shard_map(local_block, mesh=mesh, in_specs=in_specs, out_specs=row_spec, check_vma=False)
```

```python
import functools

import jax
import jax.numpy as jnp
from jax import lax
from jax.experimental import pallas as pl
from jax.experimental.pallas import tpu as pltpu
from jax.sharding import PartitionSpec as P

NORM_EPS = 1e-6
ROUTE_SCALE = 2.5
GROUPS = 8
GROUP_LIMIT = 4
F32 = jnp.float32
BF16 = jnp.bfloat16
VMEM_LIMIT = 67_000_000
TILE = 16


def dot_f32(a, b):
    return jnp.dot(a, b, preferred_element_type=F32)


def place():
    me = lax.axis_index("ep")
    core = lax.rem(me, 2)
    x = lax.rem(me // 2, 2)
    y = me // 4
    return me, core, x, y, me + 1 - 2 * core, me + 2 - 4 * x, me + 4 - 8 * y


def pos_of(dev):
    return lax.rem(dev, 2) * 4 + dev // 2


def rcopy(src, dst, ssem, rsem, dev):
    return pltpu.make_async_remote_copy(
        src_ref=src, dst_ref=dst, send_sem=ssem, recv_sem=rsem, device_id={"ep": dev}, device_id_type=pl.DeviceIdType.MESH
    )


def split3(v):
    hi = v.astype(BF16)
    rest = v - hi.astype(F32)
    mid = rest.astype(BF16)
    return hi, mid, (rest - mid.astype(F32)).astype(BF16)


def iota(shape, axis):
    return lax.broadcasted_iota(jnp.int32, shape, axis)


def gather_up_kernel(
    n_kc, hid_ref, gain_ref, rw_ref, ids_ref, wg_ref, wu_ref, h_ref, rg_ref, xn_ref, tab_ref, back_ref,
    xall, pick, xsrc, acc, wbuf, hbuf, xe, meta_s, meta_r, ids_r, tab_v, tab_s,
    sid, cid, ids_t, w_sem, h_sem, t_sem, x_sem, i_send, i_recv, m_send, m_recv, a_send, a_recv,
):
    me, core, x, y, sib, xnb, ynb = place()
    tok, dim = hid_ref.shape
    n_exp, _, inter = wg_ref.shape
    cap = h_ref.shape[1]
    kw = dim // n_kc
    half = tok // 2
    n_steps = n_exp * n_kc
    slots = wbuf.shape[0]
    n_et = cap // TILE
    n_st = pick.shape[1] // TILE

    def w_copies(s):
        e, kc, slot = lax.rem(s, n_exp), s // n_exp, lax.rem(s, slots)
        rows = pl.ds(pl.multiple_of(kc * kw, kw), kw)
        return (
            pltpu.make_async_copy(wg_ref.at[e, rows, :], wbuf.at[slot, :, pl.ds(0, inter)], w_sem.at[slot, 0]),
            pltpu.make_async_copy(wu_ref.at[e, rows, :], wbuf.at[slot, :, pl.ds(inter, inter)], w_sem.at[slot, 1]),
        )

    def w_start(s):
        for c in w_copies(s):
            c.start()

    for s in range(slots - 1):
        w_start(jnp.int32(s))

    ids_t[...] = jnp.full(ids_t.shape, -1, jnp.int32)
    ids_t[: ids_ref.shape[0], :tok] = ids_ref[...]

    barrier = pltpu.get_barrier_semaphore()
    for k in range(1, 8):
        pl.semaphore_signal(barrier, inc=1, device_id={"ep": lax.rem(me + k, 8)}, device_id_type=pl.DeviceIdType.MESH)

    x_f32 = hid_ref[...].astype(F32)
    inv_rms = lax.rsqrt(jnp.mean(x_f32 * x_f32, axis=-1, keepdims=True) + NORM_EPS)
    x_norm = (x_f32 * inv_rms * gain_ref[...]).astype(BF16)
    my_pos = pos_of(me)
    my_rows = pl.ds(pl.multiple_of(my_pos * tok, tok), tok)
    for kc in range(n_kc):
        xall[kc, my_rows, :] = x_norm[:, kc * kw : (kc + 1) * kw]

    def xn_copy(kc):
        return pltpu.make_async_copy(xall.at[kc, my_rows, :], xn_ref.at[:, pl.ds(kc * kw, kw)], x_sem.at[kc])

    for kc in range(n_kc):
        xn_copy(kc).start()
    pl.semaphore_wait(barrier, 7)

    def block(kc, dev, part=None):
        start = pos_of(dev) * tok + (0 if part is None else part * half)
        n = tok if part is None else half
        return xall.at[kc, pl.ds(pl.multiple_of(start, half), n), :]

    def send(kc, kind, dev_src, to, part=None):
        ref = block(kc, dev_src, part)
        return rcopy(ref, ref, a_send.at[kc, kind], a_recv.at[kc, kind], to)

    diag = me + 6 - 4 * x - 8 * y
    kinds = (
        (me, sib, None), (me, xnb, None), (me, ynb, None), (xnb, ynb, 0), (ynb, xnb, 1),
        (xnb, sib, None), (ynb, sib, None), (diag, sib, 0), (diag, sib, 1),
    )

    def copy(kc, kind):
        src, to, part = kinds[kind]
        return send(kc, kind, src, to, part)

    def start(kc, which):
        for kind in which:
            copy(kc, kind).start()

    def received(kc, which):
        for kind in which:
            copy(kc, kind).wait_recv()

    def serve_a(kc):
        received(kc, (1, 2))
        start(kc, (3, 4, 5, 6))
        pl.when(kc + 1 < n_kc)(lambda: start(kc + 1, (1, 2, 0)))

    def serve_b(kc):
        received(kc, (3, 4))
        start(kc, (7, 8))

    def meta(k):
        to = lax.rem(me + k, 8)
        return rcopy(meta_s.at[to], meta_r.at[my_pos], m_send.at[k], m_recv.at[k], to)

    def ids_copy(k):
        return rcopy(ids_t, ids_r.at[my_pos], i_send.at[k], i_recv.at[k], lax.rem(me + k, 8))

    for k in range(1, 8):
        ids_copy(k).start()
    start(0, (1, 2, 0))
    ids_r[pl.ds(my_pos, 1)] = ids_t[...].reshape(1, 8, 256)

    parts = lax.dot_general(
        jnp.concatenate(split3(rw_ref[...]), axis=0), x_norm, (((1,), (1,)), ((), ())), preferred_element_type=F32
    )
    logits = parts[:64] + (parts[64:128] + parts[128:192])
    scores = jax.nn.sigmoid(logits)
    exp_iota = iota(scores.shape, 0)
    chosen = exp_iota == ids_t[0:1, :tok]
    for j in range(1, 6):
        chosen = chosen | (exp_iota == ids_t[j : j + 1, :tok])
    picked = jnp.where(chosen, scores, 0.0)
    gates = ROUTE_SCALE * picked / jnp.sum(picked, axis=0, keepdims=True)
    meta_s[...] = jnp.zeros(meta_s.shape, F32)
    for d in range(8):
        meta_s[d, :, 0:tok] = gates[d * n_exp : (d + 1) * n_exp, :]
    meta_r[pl.ds(my_pos, 1)] = meta_s[pl.ds(me, 1)]
    for k in range(1, 8):
        meta(k).start()
    for k in range(1, 8):
        ids_copy(k).wait_recv()

    my_exp = me * n_exp + iota((n_exp, 256), 0)
    masks = []
    for s in range(8):
        hit = my_exp == ids_r[s, 0:1, :]
        for j in range(1, 6):
            hit = hit | (my_exp == ids_r[s, j : j + 1, :])
        masks.append(hit)
    ones = jnp.concatenate([jnp.where(m, 1.0, 0.0) for m in masks], axis=0).astype(BF16)
    upper = iota((256, 256), 0) <= iota((256, 256), 1)
    cums = dot_f32(ones, jnp.where(upper, 1.0, 0.0).astype(BF16))
    cums = [cums[s * n_exp : (s + 1) * n_exp] for s in range(8)]

    lane = iota((n_exp, 128), 1)
    base = jnp.zeros((n_exp, 128), F32)
    count = jnp.zeros((n_exp, 128), F32)
    before = jnp.zeros((n_exp, 1), F32)
    for s in range(8):
        n = cums[s][:, 255:256]
        base = jnp.where(lane == s, before, base)
        count = jnp.where(lane == s, n, count)
        before = before + n
    base, count = base.astype(jnp.int32), count.astype(jnp.int32)
    first = base // TILE
    tiles = jnp.where(count > 0, (base + count - 1) // TILE - first + 1, 0)
    sub = iota((n_exp, 128), 0)
    ends = tiles
    for d in (1, 2, 4):
        ends = ends + jnp.where(sub >= d, pltpu.roll(ends, d, 0), 0)
    begin = ends - tiles
    shift = ((begin - first) * TILE + base).astype(F32)

    for s in range(8):
        slot_id = jnp.where(masks[s], cums[s] - 1.0 + shift[:, s : s + 1], -1.0)
        sid[s] = slot_id
        by_col = jnp.full((8, 256), -1.0, F32)
        for e in range(n_exp):
            by_col = jnp.where(ids_r[s] == me * n_exp + e, slot_id[e : e + 1], by_col)
        cid[s] = by_col

    def build(s, carry):
        for q in range(0, n_st * TILE, 128):
            want = (iota((128, 256), 0) + q).astype(F32)
            got = want == cid[s, 0:1, :]
            for j in range(1, 6):
                got = got | (want == cid[s, j : j + 1, :])
            pick[s, q : q + 128, :] = jnp.where(got, 1.0, 0.0).astype(BF16)[:, :tok]
        return carry

    lax.fori_loop(0, 4, build, 0)
    serve_a(0)
    lax.fori_loop(4, 8, build, 0)

    rows24 = jnp.concatenate([first, tiles, begin], axis=0).astype(F32).astype(BF16)
    src = iota((128, 768), 0)
    col = iota((128, 768), 1)
    spread = jnp.where(jnp.where(col < 256, col % 8, (col - 256) // 64) == src, 1.0, 0.0).astype(BF16)
    table = dot_f32(rows24, spread).astype(jnp.int32)
    t_first, t_tiles, t_begin = table[:n_exp], table[n_exp : 2 * n_exp], table[2 * n_exp :]
    col = iota((n_exp, 256), 1)
    nth = col // 8 - t_first[:, :256]
    valid = (nth >= 0) & (nth < t_tiles[:, :256])
    tab_v[...] = jnp.where(valid, t_begin[:, :256] + nth, n_st - 1)
    out = pltpu.make_async_copy(tab_v, tab_ref, t_sem.at[0])
    out.start()
    nth = iota((n_exp, 512), 1) % 64 - t_begin[:, 256:]
    valid = (nth >= 0) & (nth < t_tiles[:, 256:])
    back = jnp.where(valid, iota((n_exp, 512), 0) * n_et + t_first[:, 256:] + nth, 0)
    back_ref[...] = jnp.sum(back, axis=0, keepdims=True)
    out.wait()
    load = pltpu.make_async_copy(tab_ref, tab_s, t_sem.at[1])
    load.start()

    load.wait()

    def select(kc):
        received(kc, (0, 5, 6, 7, 8))

        for s in range(8):
            for n in range(0, kw, 256):
                res = dot_f32(pick[s], xall[kc, s * tok : (s + 1) * tok, n : n + 256]).astype(BF16)
                xsrc[s * n_st : (s + 1) * n_st, :, n : n + 256] = res.reshape(n_st, TILE, 256)

    def fill(s):
        e, slot = lax.rem(s, n_exp), lax.rem(s, 2)
        for t in range(n_et):
            got = [xsrc[k * n_st + (tab_s[e, t * 8 + k] & 63)] for k in range(8)]
            while len(got) > 1:
                got = [got[i] + got[i + 1] for i in range(0, len(got), 2)]
            xe[slot, t * TILE : (t + 1) * TILE, :] = got[0]

    serve_b(0)
    select(0)
    fill(jnp.int32(0))

    def step(s, carry):
        e, kc = lax.rem(s, n_exp), s // n_exp
        slot = lax.rem(s, slots)
        more = kc + 1 < n_kc
        pl.when(more & (e == 2))(lambda: serve_a(kc + 1))
        pl.when(more & (e == 5))(lambda: serve_b(kc + 1))
        pl.when(more & (e == n_exp - 1))(lambda: select(kc + 1))

        @pl.when(s + slots - 1 < n_steps)
        def _():
            w_start(s + slots - 1)

        for c in w_copies(s):
            c.wait()
        fill(s + 1)
        for n in range(0, 2 * inter, 256):
            part = dot_f32(xe[lax.rem(s, 2)], wbuf[slot, :, n : n + 256])
            acc[e, :, n : n + 256] = jnp.where(kc > 0, acc[e, :, n : n + 256], 0.0) + part

        @pl.when(kc == n_kc - 1)
        def _():
            b = lax.rem(e, 2)

            @pl.when(e >= 2)
            def _():
                pltpu.make_async_copy(hbuf.at[b], h_ref.at[e - 2], h_sem.at[b]).wait()

            for n in range(0, inter, 128):
                g = acc[e, :, n : n + 128]
                u = acc[e, :, inter + n : inter + n + 128]
                hbuf[b, :, n : n + 128] = (jax.nn.silu(g) * u).astype(BF16)
            pltpu.make_async_copy(hbuf.at[b], h_ref.at[e], h_sem.at[b]).start()

        return carry

    lax.fori_loop(0, n_steps, step, 0)

    for e in range(n_exp - 2, n_exp):
        pltpu.make_async_copy(hbuf.at[e % 2], h_ref.at[e], h_sem.at[e % 2]).wait()
    for k in range(1, 8):
        meta(k).wait_recv()
    for s in range(8):
        rg_ref[s, :n_exp] = sid[s]
        rg_ref[s, n_exp:] = meta_r[s]
    for kc in range(n_kc):
        xn_copy(kc).wait()
    for k in range(1, 8):
        ids_copy(k).wait_send()
        meta(k).wait_send()
    for kc in range(n_kc):
        for kind in range(len(kinds)):
            copy(kc, kind).wait_send()


def down_kernel(
    n_chunk, hid_ref, xn_ref, rg_ref, back_ref, h_ref, wd_ref, wsg_ref, wsu_ref, wsd_ref, out_ref,
    hv, weigh, wdb, etile, esrc, part, got0, mid, got1, quart, got2, total, wsb, wdsb, hs,
    hv_sem, wd_sem, ws_sem, wds_sem, d_send, d_recv, p_send, p_recv, q_send, q_recv,
):
    me, core, x, y, sib, xnb, ynb = place()
    n_exp, cap, inter = h_ref.shape
    tok, dim = hid_ref.shape
    n_et = cap // TILE
    n_slot = weigh.shape[-1]
    n_st = n_slot // TILE
    cw = dim // n_chunk
    hw = cw // 2
    unroll = 2
    n_down = n_exp // unroll
    per_src = 4
    per_chunk = n_down + 8 // per_src + 2
    n_steps = n_chunk * per_chunk
    slots = wdb.shape[0]
    sw = wsb.shape[-1] // 2
    n_s = wsg_ref.shape[1] // sw
    dw = wdsb.shape[-1]
    n_d = dim // dw

    def wd_copy(i):
        e, n, slot = lax.rem(i, n_exp), i // n_exp, lax.rem(i, slots)
        return pltpu.make_async_copy(wd_ref.at[e, :, pl.ds(pl.multiple_of(n * cw, cw), cw)], wdb.at[slot], wd_sem.at[slot])

    def h_copy(e):
        return pltpu.make_async_copy(h_ref.at[e], hv.at[e], hv_sem.at[e])

    def ws_copies(i):
        cols = pl.ds(pl.multiple_of(i * sw, sw), sw)
        slot = lax.rem(i, wsb.shape[0])
        return (
            pltpu.make_async_copy(wsg_ref.at[:, cols], wsb.at[slot, :, pl.ds(0, sw)], ws_sem.at[slot, 0]),
            pltpu.make_async_copy(wsu_ref.at[:, cols], wsb.at[slot, :, pl.ds(sw, sw)], ws_sem.at[slot, 1]),
        )

    def wds_copy(i):
        slot = lax.rem(i, 2)
        return pltpu.make_async_copy(wsd_ref.at[:, pl.ds(pl.multiple_of(i * dw, dw), dw)], wdsb.at[slot], wds_sem.at[slot])

    def start(copies):
        for c in copies:
            c.start()

    def wait(copies):
        for c in copies:
            c.wait()

    h_copy(0).start()
    for i in range(slots - unroll):
        wd_copy(jnp.int32(i)).start()
    for e in range(1, n_exp):
        h_copy(e).start()
    for i in range(wsb.shape[0] - 1):
        start(ws_copies(jnp.int32(i)))

    barrier = pltpu.get_barrier_semaphore()
    for dev in (sib, xnb, ynb):
        pl.semaphore_signal(barrier, inc=1, device_id={"ep": dev}, device_id_type=pl.DeviceIdType.MESH)

    def build(s, carry):
        slot = iota((tok, n_slot), 1).astype(F32)
        val = jnp.zeros((tok, n_slot), F32)
        cols = jnp.concatenate([rg_ref[s], jnp.zeros((128 - 2 * n_exp, 256), F32)], axis=0).T[:tok]
        for e in range(n_exp):
            val = jnp.where(cols[:, e : e + 1] == slot, cols[:, n_exp + e : n_exp + e + 1], val)
        for k, piece in enumerate(split3(val)):
            weigh[s, k * tok : (k + 1) * tok, :] = piece
        return carry

    lax.fori_loop(0, 8, build, 0)
    pl.semaphore_wait(barrier, 3)

    def d_copy(n):
        b = lax.rem(n, 2)
        return rcopy(part.at[b, :, 1 - core], got0.at[b], d_send.at[b], d_recv.at[b], sib)

    def p_copies(n):
        b = lax.rem(n, 4)
        return (
            rcopy(mid.at[b, 0, :, 1 - x], got1.at[b, 0], p_send.at[b, 0], p_recv.at[b, 0], xnb),
            rcopy(mid.at[b, 1, 1 - y], got1.at[b, 1], p_send.at[b, 1], p_recv.at[b, 1], ynb),
        )

    def q_copies(n):
        b = lax.rem(n, 4)
        return (
            rcopy(quart.at[b, 0, 1 - y], got2.at[b, 0], q_send.at[b, 0], q_recv.at[b, 0], ynb),
            rcopy(quart.at[b, 1, 1 - x], got2.at[b, 1], q_send.at[b, 1], q_recv.at[b, 1], xnb),
        )

    def stage_p(n):
        b, b4 = lax.rem(n, 2), lax.rem(n, 4)
        d_copy(n).wait()
        for hf in range(2):
            for yy in range(2):
                for xx in range(2):
                    rows = pl.ds((yy * 2 + xx) * tok, tok)
                    mid[b4, hf, yy, xx] = part[b, hf, core, rows, :] + got0[b, hf, rows, :]
        start(p_copies(n))

    def stage_q(n):
        b = lax.rem(n, 4)
        wait(p_copies(n))
        for k in range(2):
            quart[b, 0, k] = mid[b, 0, k, x] + got1[b, 0, k]
            quart[b, 1, k] = mid[b, 1, y, k] + got1[b, 1, k]
        start(q_copies(n))

    def stage_f(n):
        b = lax.rem(n, 4)
        wait(q_copies(n))
        total[n, 0] = quart[b, 0, y] + got2[b, 0]
        total[n, 1] = quart[b, 1, x] + got2[b, 1]

    def down(n, j):
        i0 = n * n_exp + j * unroll
        for u in range(unroll):
            i = i0 + slots - unroll + u

            @pl.when(i < n_chunk * n_exp)
            def _():
                wd_copy(i).start()

        @pl.when(n == 0)
        def _():
            for u in range(unroll):
                h_copy(j * unroll + u).wait()

        for u in range(unroll):
            wd_copy(i0 + u).wait()
        for u in range(unroll):
            e = j * unroll + u
            res = dot_f32(hv[e], wdb[lax.rem(i0 + u, slots)]).astype(BF16)
            etile[pl.ds(e * n_et, n_et)] = res.reshape(n_et, TILE, cw)

    def combine(n, g):
        b = lax.rem(n, 2)
        for u in range(per_src):
            s = g * per_src + u
            for t in range(n_st):
                esrc[u, t * TILE : (t + 1) * TILE, :] = etile[back_ref[0, s * 64 + t]]
        for u in range(per_src):
            s = g * per_src + u
            res = dot_f32(weigh[s], esrc[u])
            res = res[:tok] + (res[tok : 2 * tok] + res[2 * tok :])
            for hf in range(2):
                part[b, hf, s // 4, pl.ds(pl.multiple_of(lax.rem(s, 4) * tok, tok), tok), :] = res[:, hf * hw : (hf + 1) * hw]

    def shared_up(i):
        ahead = i + wsb.shape[0] - 1

        @pl.when(ahead < n_s)
        def _():
            start(ws_copies(ahead))

        wait(ws_copies(i))
        both = dot_f32(xn_ref[...], wsb[lax.rem(i, wsb.shape[0])])
        hs[i] = (jax.nn.silu(both[:, :sw]) * both[:, sw:]).astype(BF16)

    def step(s, carry):
        n, j = s // per_chunk, lax.rem(s, per_chunk)
        pl.when(j < n_down)(lambda: down(n, j))

        @pl.when((j >= n_down) & (j < per_chunk - 2))
        def _():
            combine(n, j - n_down)

        pl.when(j == per_chunk - 3)(lambda: d_copy(n).start())
        i = n * 2 + j - (per_chunk - 2)
        pl.when((j >= per_chunk - 2) & (i < n_s))(lambda: shared_up(i))

        @pl.when(j == 0)
        def _():
            pl.when(n >= 1)(lambda: stage_p(n - 1))
            pl.when(n >= 4)(lambda: stage_f(n - 4))

        pl.when((j == n_down - 1) & (n >= 2))(lambda: stage_q(n - 2))

        return carry

    lax.fori_loop(0, n_steps, step, 0)

    last = jnp.int32(n_chunk - 1)
    wds_copy(jnp.int32(0)).start()
    stage_p(last)
    stage_q(last - 1)
    stage_f(last - 3)
    stage_f(last - 2)
    for i in range(n_d):
        if i + 1 < n_d:
            wds_copy(jnp.int32(i + 1)).start()
        wds_copy(jnp.int32(i)).wait()
        res = jnp.zeros((tok, dw), F32)
        for k in range(n_s):
            res = res + dot_f32(hs[k], wdsb[i % 2, k * sw : (k + 1) * sw, :])
        out_ref[:, i * dw : (i + 1) * dw] = res.astype(BF16)
    stage_f(last - 1)
    stage_q(last)
    stage_f(last)
    for n in range(n_chunk):
        for hf in range(2):
            cols = slice(n * cw + hf * hw, n * cw + (hf + 1) * hw)
            out_ref[:, cols] = (hid_ref[:, cols].astype(F32) + out_ref[:, cols].astype(F32) + total[n, hf]).astype(BF16)


def solution(mesh):
    ep_size = mesh.shape["ep"]
    assert ep_size == 8

    def local_block(hidden_in, norm_gain, router_w, w_gate, w_up, w_down, ws_gate, ws_up, ws_down, expert_ids):
        tok, top_k = expert_ids.shape
        dim = hidden_in.shape[1]
        n_exp, _, inter = w_gate.shape
        s_inter = ws_gate.shape[1]
        cap = GROUPS * ((top_k + GROUP_LIMIT - 1) // GROUP_LIMIT) * tok // n_exp
        n_kc, slots = 4, 3
        kw = dim // n_kc
        pair_cap = cap * n_exp // ep_size
        n_st = (pair_cap + 14 * n_exp) // TILE + n_exp
        n_slot = -(-(n_st + 1) * TILE // 128) * 128
        n_st = n_slot // TILE
        assert n_st <= 64
        vmem = pl.BlockSpec(memory_space=pltpu.VMEM)
        smem = pl.BlockSpec(memory_space=pltpu.SMEM)
        hbm = pl.BlockSpec(memory_space=pl.ANY)
        dma = pltpu.SemaphoreType.DMA
        h, rg, xn, _, back = pl.pallas_call(
            functools.partial(gather_up_kernel, n_kc),
            out_shape=(
                jax.ShapeDtypeStruct((n_exp, cap, inter), BF16),
                jax.ShapeDtypeStruct((8, 2 * n_exp, 256), F32),
                jax.ShapeDtypeStruct((tok, dim), BF16),
                jax.ShapeDtypeStruct((n_exp, 256), jnp.int32),
                jax.ShapeDtypeStruct((1, 512), jnp.int32),
            ),
            in_specs=[vmem, vmem, vmem, vmem, hbm, hbm],
            out_specs=(hbm, vmem, hbm, hbm, vmem),
            scratch_shapes=[
                pltpu.VMEM((n_kc, 8 * tok, kw), BF16),
                pltpu.VMEM((8, n_slot, tok), BF16),
                pltpu.VMEM((7 * n_st + 64, TILE, kw), BF16),
                pltpu.VMEM((n_exp, cap, 2 * inter), F32),
                pltpu.VMEM((slots, kw, 2 * inter), BF16),
                pltpu.VMEM((2, cap, inter), BF16),
                pltpu.VMEM((2, cap, kw), BF16),
                pltpu.VMEM((8, n_exp, 256), F32),
                pltpu.VMEM((8, n_exp, 256), F32),
                pltpu.VMEM((8, 8, 256), jnp.int32),
                pltpu.VMEM((n_exp, 256), jnp.int32),
                pltpu.SMEM((n_exp, 256), jnp.int32),
                pltpu.VMEM((8, n_exp, 256), F32),
                pltpu.VMEM((8, n_exp, 256), F32),
                pltpu.VMEM((8, 256), jnp.int32),
                dma((slots, 2)),
                dma((2,)),
                dma((2,)),
                dma((n_kc,)),
                dma((8,)),
                dma((8,)),
                dma((8,)),
                dma((8,)),
                dma((n_kc, 9)),
                dma((n_kc, 9)),
            ],
            compiler_params=pltpu.CompilerParams(collective_id=0, has_side_effects=True, vmem_limit_bytes=VMEM_LIMIT),
            name="gather_up",
        )(hidden_in, norm_gain.reshape(1, dim), router_w, expert_ids.T, w_gate, w_up)

        n_chunk, dslots = 8, 14
        cw = dim // n_chunk
        hw = cw // 2
        sw, dw = 256, 512
        return pl.pallas_call(
            functools.partial(down_kernel, n_chunk),
            out_shape=jax.ShapeDtypeStruct((tok, dim), BF16),
            in_specs=[vmem, vmem, vmem, smem, hbm, hbm, hbm, hbm, hbm],
            out_specs=vmem,
            scratch_shapes=[
                pltpu.VMEM((n_exp, cap, inter), BF16),
                pltpu.VMEM((8, 3 * tok, n_slot), BF16),
                pltpu.VMEM((dslots, inter, cw), BF16),
                pltpu.VMEM((n_exp * cap // TILE, TILE, cw), BF16),
                pltpu.VMEM((4, n_slot, cw), BF16),
                pltpu.VMEM((2, 2, 2, 4 * tok, hw), F32),
                pltpu.VMEM((2, 2, 4 * tok, hw), F32),
                pltpu.VMEM((4, 2, 2, 2, tok, hw), F32),
                pltpu.VMEM((4, 2, 2, tok, hw), F32),
                pltpu.VMEM((4, 2, 2, tok, hw), F32),
                pltpu.VMEM((4, 2, tok, hw), F32),
                pltpu.VMEM((n_chunk, 2, tok, hw), F32),
                pltpu.VMEM((3, dim, 2 * sw), BF16),
                pltpu.VMEM((2, s_inter, dw), BF16),
                pltpu.VMEM((s_inter // sw, tok, sw), BF16),
                dma((n_exp,)),
                dma((dslots,)),
                dma((3, 2)),
                dma((2,)),
                dma((2,)),
                dma((2,)),
                dma((4, 2)),
                dma((4, 2)),
                dma((4, 2)),
                dma((4, 2)),
            ],
            compiler_params=pltpu.CompilerParams(collective_id=1, has_side_effects=True, vmem_limit_bytes=VMEM_LIMIT),
            name="down_sum",
        )(hidden_in, xn, rg, back, h, w_down, ws_gate, ws_up, ws_down)

    row_spec = P(("dp", "ep"), None)
    in_specs = (row_spec, P(), P(), P("ep"), P("ep"), P("ep"), P(), P(), P(), row_spec)
    return jax.shard_map(local_block, mesh=mesh, in_specs=in_specs, out_specs=row_spec, check_vma=False)
```

```python
import functools

import jax
import jax.numpy as jnp
from jax import lax
from jax.experimental import pallas as pl
from jax.experimental.pallas import tpu as pltpu
from jax.sharding import PartitionSpec as P

NORM_EPS = 1e-6
ROUTE_SCALE = 2.5
GROUPS = 8
GROUP_LIMIT = 4
F32 = jnp.float32
BF16 = jnp.bfloat16
VMEM_LIMIT = 67_000_000
TILE = 16


def dot_f32(a, b):
    return jnp.dot(a, b, preferred_element_type=F32)


def place():
    me = lax.axis_index("ep")
    core = lax.rem(me, 2)
    x = lax.rem(me // 2, 2)
    y = me // 4
    return me, core, x, y, me + 1 - 2 * core, me + 2 - 4 * x, me + 4 - 8 * y


def pos_of(dev):
    return lax.rem(dev, 2) * 4 + dev // 2


def rcopy(src, dst, ssem, rsem, dev):
    return pltpu.make_async_remote_copy(
        src_ref=src, dst_ref=dst, send_sem=ssem, recv_sem=rsem, device_id={"ep": dev}, device_id_type=pl.DeviceIdType.MESH
    )


def split3(v):
    hi = v.astype(BF16)
    rest = v - hi.astype(F32)
    mid = rest.astype(BF16)
    return hi, mid, (rest - mid.astype(F32)).astype(BF16)


def iota(shape, axis):
    return lax.broadcasted_iota(jnp.int32, shape, axis)


def gather_up_kernel(
    n_kc, hid_ref, gain_ref, rw_ref, ids_ref, wg_ref, wu_ref, h_ref, rg_ref, xn_ref, tab_ref, back_ref,
    xall, pick, xsrc, acc, wbuf, hbuf, xe, meta_s, meta_r, ids_r, tab_v, tab_s,
    sid, cid, ids_t, w_sem, h_sem, t_sem, x_sem, i_send, i_recv, m_send, m_recv, a_send, a_recv,
):
    me, core, x, y, sib, xnb, ynb = place()
    tok, dim = hid_ref.shape
    n_exp, _, inter = wg_ref.shape
    cap = h_ref.shape[1]
    kw = dim // n_kc
    half = tok // 2
    n_steps = n_exp * n_kc
    slots = wbuf.shape[0]
    n_et = cap // TILE
    n_st = pick.shape[1] // TILE

    def w_copies(s):
        e, kc, slot = lax.rem(s, n_exp), s // n_exp, lax.rem(s, slots)
        rows = pl.ds(pl.multiple_of(kc * kw, kw), kw)
        return (
            pltpu.make_async_copy(wg_ref.at[e, rows, :], wbuf.at[slot, :, pl.ds(0, inter)], w_sem.at[slot, 0]),
            pltpu.make_async_copy(wu_ref.at[e, rows, :], wbuf.at[slot, :, pl.ds(inter, inter)], w_sem.at[slot, 1]),
        )

    def w_start(s):
        for c in w_copies(s):
            c.start()

    for s in range(slots - 1):
        w_start(jnp.int32(s))

    ids_t[...] = jnp.full(ids_t.shape, -1, jnp.int32)
    ids_t[: ids_ref.shape[0], :tok] = ids_ref[...]

    barrier = pltpu.get_barrier_semaphore()
    for k in range(1, 8):
        pl.semaphore_signal(barrier, inc=1, device_id={"ep": lax.rem(me + k, 8)}, device_id_type=pl.DeviceIdType.MESH)

    x_f32 = hid_ref[...].astype(F32)
    inv_rms = lax.rsqrt(jnp.mean(x_f32 * x_f32, axis=-1, keepdims=True) + NORM_EPS)
    x_norm = (x_f32 * inv_rms * gain_ref[...]).astype(BF16)
    my_pos = pos_of(me)
    my_rows = pl.ds(pl.multiple_of(my_pos * tok, tok), tok)
    for kc in range(n_kc):
        xall[kc, my_rows, :] = x_norm[:, kc * kw : (kc + 1) * kw]

    def xn_copy(kc):
        return pltpu.make_async_copy(xall.at[kc, my_rows, :], xn_ref.at[:, pl.ds(kc * kw, kw)], x_sem.at[kc])

    for kc in range(n_kc):
        xn_copy(kc).start()
    pl.semaphore_wait(barrier, 7)

    def block(kc, dev, part=None):
        start = pos_of(dev) * tok + (0 if part is None else part * half)
        n = tok if part is None else half
        return xall.at[kc, pl.ds(pl.multiple_of(start, half), n), :]

    def send(kc, kind, dev_src, to, part=None):
        ref = block(kc, dev_src, part)
        return rcopy(ref, ref, a_send.at[kc, kind], a_recv.at[kc, kind], to)

    diag = me + 6 - 4 * x - 8 * y
    kinds = (
        (me, sib, None), (me, xnb, None), (me, ynb, None), (xnb, ynb, 0), (ynb, xnb, 1),
        (xnb, sib, None), (ynb, sib, None), (diag, sib, 0), (diag, sib, 1),
    )

    def copy(kc, kind):
        src, to, part = kinds[kind]
        return send(kc, kind, src, to, part)

    def start(kc, which):
        for kind in which:
            copy(kc, kind).start()

    def received(kc, which):
        for kind in which:
            copy(kc, kind).wait_recv()

    def serve_a(kc):
        received(kc, (1, 2))
        start(kc, (3, 4, 5, 6))
        pl.when(kc + 1 < n_kc)(lambda: start(kc + 1, (1, 2, 0)))

    def serve_b(kc):
        received(kc, (3, 4))
        start(kc, (7, 8))

    def meta(k):
        to = lax.rem(me + k, 8)
        return rcopy(meta_s.at[to], meta_r.at[my_pos], m_send.at[k], m_recv.at[k], to)

    def ids_copy(k):
        return rcopy(ids_t, ids_r.at[my_pos], i_send.at[k], i_recv.at[k], lax.rem(me + k, 8))

    for k in range(1, 8):
        ids_copy(k).start()
    start(0, (1, 2, 0))
    ids_r[pl.ds(my_pos, 1)] = ids_t[...].reshape(1, 8, 256)

    parts = lax.dot_general(
        jnp.concatenate(split3(rw_ref[...]), axis=0), x_norm, (((1,), (1,)), ((), ())), preferred_element_type=F32
    )
    logits = parts[:64] + (parts[64:128] + parts[128:192])
    scores = jax.nn.sigmoid(logits)
    exp_iota = iota(scores.shape, 0)
    chosen = exp_iota == ids_t[0:1, :tok]
    for j in range(1, 6):
        chosen = chosen | (exp_iota == ids_t[j : j + 1, :tok])
    picked = jnp.where(chosen, scores, 0.0)
    gates = ROUTE_SCALE * picked / jnp.sum(picked, axis=0, keepdims=True)
    meta_s[...] = jnp.zeros(meta_s.shape, F32)
    for d in range(8):
        meta_s[d, :, 0:tok] = gates[d * n_exp : (d + 1) * n_exp, :]
    meta_r[pl.ds(my_pos, 1)] = meta_s[pl.ds(me, 1)]
    for k in range(1, 8):
        meta(k).start()
    for k in range(1, 8):
        ids_copy(k).wait_recv()

    my_exp = me * n_exp + iota((n_exp, 256), 0)
    masks = []
    for s in range(8):
        hit = my_exp == ids_r[s, 0:1, :]
        for j in range(1, 6):
            hit = hit | (my_exp == ids_r[s, j : j + 1, :])
        masks.append(hit)
    ones = jnp.concatenate([jnp.where(m, 1.0, 0.0) for m in masks], axis=0).astype(BF16)
    upper = iota((256, 256), 0) <= iota((256, 256), 1)
    cums = dot_f32(ones, jnp.where(upper, 1.0, 0.0).astype(BF16))
    cums = [cums[s * n_exp : (s + 1) * n_exp] for s in range(8)]

    lane = iota((n_exp, 128), 1)
    base = jnp.zeros((n_exp, 128), F32)
    count = jnp.zeros((n_exp, 128), F32)
    before = jnp.zeros((n_exp, 1), F32)
    for s in range(8):
        n = cums[s][:, 255:256]
        base = jnp.where(lane == s, before, base)
        count = jnp.where(lane == s, n, count)
        before = before + n
    base, count = base.astype(jnp.int32), count.astype(jnp.int32)
    first = base // TILE
    tiles = jnp.where(count > 0, (base + count - 1) // TILE - first + 1, 0)
    sub = iota((n_exp, 128), 0)
    ends = tiles
    for d in (1, 2, 4):
        ends = ends + jnp.where(sub >= d, pltpu.roll(ends, d, 0), 0)
    begin = ends - tiles
    shift = ((begin - first) * TILE + base).astype(F32)

    for s in range(8):
        slot_id = jnp.where(masks[s], cums[s] - 1.0 + shift[:, s : s + 1], -1.0)
        sid[s] = slot_id
        by_col = jnp.full((8, 256), -1.0, F32)
        for e in range(n_exp):
            by_col = jnp.where(ids_r[s] == me * n_exp + e, slot_id[e : e + 1], by_col)
        cid[s] = by_col

    rows24 = jnp.concatenate([first, tiles, begin], axis=0).astype(F32).astype(BF16)
    src = iota((128, 768), 0)
    col = iota((128, 768), 1)
    spread = jnp.where(jnp.where(col < 256, col % 8, (col - 256) // 64) == src, 1.0, 0.0).astype(BF16)
    table = dot_f32(rows24, spread).astype(jnp.int32)
    t_first, t_tiles, t_begin = table[:n_exp], table[n_exp : 2 * n_exp], table[2 * n_exp :]
    col = iota((n_exp, 256), 1)
    nth = col // 8 - t_first[:, :256]
    valid = (nth >= 0) & (nth < t_tiles[:, :256])
    tab_v[...] = jnp.where(valid, t_begin[:, :256] + nth, n_st - 1)
    out = pltpu.make_async_copy(tab_v, tab_ref, t_sem.at[0])
    out.start()
    nth = iota((n_exp, 512), 1) % 64 - t_begin[:, 256:]
    valid = (nth >= 0) & (nth < t_tiles[:, 256:])
    back = jnp.where(valid, iota((n_exp, 512), 0) * n_et + t_first[:, 256:] + nth, 0)
    back_ref[...] = jnp.sum(back, axis=0, keepdims=True)

    def build(s, carry):
        for q in range(0, n_st * TILE, 128):
            want = (iota((128, 256), 0) + q).astype(F32)
            got = want == cid[s, 0:1, :]
            for j in range(1, 6):
                got = got | (want == cid[s, j : j + 1, :])
            pick[s, q : q + 128, :] = jnp.where(got, 1.0, 0.0).astype(BF16)[:, :tok]
        return carry

    lax.fori_loop(0, 4, build, 0)
    out.wait()
    load = pltpu.make_async_copy(tab_ref, tab_s, t_sem.at[1])
    load.start()
    serve_a(0)
    lax.fori_loop(4, 8, build, 0)
    load.wait()

    def select(kc):
        received(kc, (0, 5, 6, 7, 8))

        for s in range(8):
            for n in range(0, kw, 256):
                res = dot_f32(pick[s], xall[kc, s * tok : (s + 1) * tok, n : n + 256]).astype(BF16)
                xsrc[s * n_st : (s + 1) * n_st, :, n : n + 256] = res.reshape(n_st, TILE, 256)

    def fill(s):
        e, slot = lax.rem(s, n_exp), lax.rem(s, 2)
        for t in range(n_et):
            got = [xsrc[k * n_st + (tab_s[e, t * 8 + k] & 63)] for k in range(8)]
            while len(got) > 1:
                got = [got[i] + got[i + 1] for i in range(0, len(got), 2)]
            xe[slot, t * TILE : (t + 1) * TILE, :] = got[0]

    serve_b(0)
    select(0)
    fill(jnp.int32(0))

    def step(s, carry):
        e, kc = lax.rem(s, n_exp), s // n_exp
        slot = lax.rem(s, slots)
        more = kc + 1 < n_kc
        pl.when(more & (e == 2))(lambda: serve_a(kc + 1))
        pl.when(more & (e == 5))(lambda: serve_b(kc + 1))
        pl.when(more & (e == n_exp - 1))(lambda: select(kc + 1))

        @pl.when(s + slots - 1 < n_steps)
        def _():
            w_start(s + slots - 1)

        for c in w_copies(s):
            c.wait()
        rows = xe.at[lax.rem(s, 2)]

        @pl.when(kc < n_kc - 1)
        def _():
            fill(s + 1)
            for n in range(0, 2 * inter, 256):
                part = dot_f32(rows[...], wbuf[slot, :, n : n + 256])
                acc[e, :, n : n + 256] = jnp.where(kc > 0, acc[e, :, n : n + 256], 0.0) + part

        @pl.when(kc == n_kc - 1)
        def _():
            b = lax.rem(e, 2)

            @pl.when(e >= 2)
            def _():
                pltpu.make_async_copy(hbuf.at[b], h_ref.at[e - 2], h_sem.at[b]).wait()

            fill(s + 1)
            for n in range(0, inter, 256):
                w = min(256, inter - n)
                g = acc[e, :, n : n + w] + dot_f32(rows[...], wbuf[slot, :, n : n + w])
                u = acc[e, :, inter + n : inter + n + w] + dot_f32(rows[...], wbuf[slot, :, inter + n : inter + n + w])
                hbuf[b, :, n : n + w] = (jax.nn.silu(g) * u).astype(BF16)
            pltpu.make_async_copy(hbuf.at[b], h_ref.at[e], h_sem.at[b]).start()

        return carry

    lax.fori_loop(0, n_steps, step, 0)

    for e in range(n_exp - 2, n_exp):
        pltpu.make_async_copy(hbuf.at[e % 2], h_ref.at[e], h_sem.at[e % 2]).wait()
    for k in range(1, 8):
        meta(k).wait_recv()
    for s in range(8):
        rg_ref[s, :n_exp] = sid[s]
        rg_ref[s, n_exp:] = meta_r[s]
    for kc in range(n_kc):
        xn_copy(kc).wait()
    for k in range(1, 8):
        ids_copy(k).wait_send()
        meta(k).wait_send()
    for kc in range(n_kc):
        for kind in range(len(kinds)):
            copy(kc, kind).wait_send()


def down_kernel(
    n_chunk, hid_ref, xn_ref, rg_ref, back_ref, h_ref, wd_ref, wsg_ref, wsu_ref, wsd_ref, out_ref,
    hv, weigh, wdb, etile, esrc, part, got0, mid, got1, quart, got2, total, wsb, wdsb, hs,
    hv_sem, wd_sem, ws_sem, wds_sem, d_send, d_recv, p_send, p_recv, q_send, q_recv,
):
    me, core, x, y, sib, xnb, ynb = place()
    n_exp, cap, inter = h_ref.shape
    tok, dim = hid_ref.shape
    n_et = cap // TILE
    n_slot = weigh.shape[-1]
    n_st = n_slot // TILE
    cw = dim // n_chunk
    hw = cw // 2
    unroll = 2
    n_down = n_exp // unroll
    per_src = 4
    per_chunk = n_down + 8 // per_src
    n_steps = n_chunk * per_chunk
    slots = wdb.shape[0]
    sw = wsb.shape[-1] // 2
    n_s = wsg_ref.shape[1] // sw
    dw = wdsb.shape[-1]
    n_d = dim // dw

    def wd_copy(i):
        e, n, slot = lax.rem(i, n_exp), i // n_exp, lax.rem(i, slots)
        return pltpu.make_async_copy(wd_ref.at[e, :, pl.ds(pl.multiple_of(n * cw, cw), cw)], wdb.at[slot], wd_sem.at[slot])

    def h_copy(e):
        return pltpu.make_async_copy(h_ref.at[e], hv.at[e], hv_sem.at[e])

    def ws_copies(i):
        cols = pl.ds(pl.multiple_of(i * sw, sw), sw)
        slot = lax.rem(i, wsb.shape[0])
        return (
            pltpu.make_async_copy(wsg_ref.at[:, cols], wsb.at[slot, :, pl.ds(0, sw)], ws_sem.at[slot, 0]),
            pltpu.make_async_copy(wsu_ref.at[:, cols], wsb.at[slot, :, pl.ds(sw, sw)], ws_sem.at[slot, 1]),
        )

    def wds_copy(i):
        slot = lax.rem(i, 2)
        return pltpu.make_async_copy(wsd_ref.at[:, pl.ds(pl.multiple_of(i * dw, dw), dw)], wdsb.at[slot], wds_sem.at[slot])

    def start(copies):
        for c in copies:
            c.start()

    def wait(copies):
        for c in copies:
            c.wait()

    h_copy(0).start()
    for i in range(slots - unroll):
        wd_copy(jnp.int32(i)).start()
    for e in range(1, n_exp):
        h_copy(e).start()
    for i in range(wsb.shape[0] - 1):
        start(ws_copies(jnp.int32(i)))
    for i in range(2):
        wds_copy(jnp.int32(i)).start()

    barrier = pltpu.get_barrier_semaphore()
    for dev in (sib, xnb, ynb):
        pl.semaphore_signal(barrier, inc=1, device_id={"ep": dev}, device_id_type=pl.DeviceIdType.MESH)

    def build(s, carry):
        slot = iota((tok, n_slot), 1).astype(F32)
        val = jnp.zeros((tok, n_slot), F32)
        cols = jnp.concatenate([rg_ref[s], jnp.zeros((128 - 2 * n_exp, 256), F32)], axis=0).T[:tok]
        for e in range(n_exp):
            val = jnp.where(cols[:, e : e + 1] == slot, cols[:, n_exp + e : n_exp + e + 1], val)
        for k, piece in enumerate(split3(val)):
            weigh[s, k * tok : (k + 1) * tok, :] = piece
        return carry

    lax.fori_loop(0, 8, build, 0)
    pl.semaphore_wait(barrier, 3)

    def d_copy(n):
        b = lax.rem(n, 2)
        return rcopy(part.at[b, :, 1 - core], got0.at[b], d_send.at[b], d_recv.at[b], sib)

    def p_copies(n):
        b = lax.rem(n, 4)
        return (
            rcopy(mid.at[lax.rem(n, 2), 0, :, 1 - x], got1.at[b, 0], p_send.at[b, 0], p_recv.at[b, 0], xnb),
            rcopy(mid.at[lax.rem(n, 2), 1, 1 - y], got1.at[b, 1], p_send.at[b, 1], p_recv.at[b, 1], ynb),
        )

    def q_copies(n):
        b = lax.rem(n, 4)
        return (
            rcopy(quart.at[b, 0, 1 - y], got2.at[b, 0], q_send.at[b, 0], q_recv.at[b, 0], ynb),
            rcopy(quart.at[b, 1, 1 - x], got2.at[b, 1], q_send.at[b, 1], q_recv.at[b, 1], xnb),
        )

    def stage_p(n):
        b = lax.rem(n, 2)
        d_copy(n).wait()
        for hf in range(2):
            for yy in range(2):
                for xx in range(2):
                    rows = pl.ds((yy * 2 + xx) * tok, tok)
                    mid[b, hf, yy, xx] = part[b, hf, core, rows, :] + got0[b, hf, rows, :]
        start(p_copies(n))

    def stage_q(n):
        b = lax.rem(n, 4)
        wait(p_copies(n))
        for k in range(2):
            quart[b, 0, k] = mid[lax.rem(n, 2), 0, k, x] + got1[b, 0, k]
            quart[b, 1, k] = mid[lax.rem(n, 2), 1, y, k] + got1[b, 1, k]
        start(q_copies(n))

    def stage_f(n):
        b = lax.rem(n, 4)
        wait(q_copies(n))
        total[n, 0] = quart[b, 0, y] + got2[b, 0]
        total[n, 1] = quart[b, 1, x] + got2[b, 1]

    def down(n, j):
        i0 = n * n_exp + j * unroll
        for u in range(unroll):
            i = i0 + slots - unroll + u

            @pl.when(i < n_chunk * n_exp)
            def _():
                wd_copy(i).start()

        @pl.when(n == 0)
        def _():
            for u in range(unroll):
                h_copy(j * unroll + u).wait()

        for u in range(unroll):
            wd_copy(i0 + u).wait()
        for u in range(unroll):
            e = j * unroll + u
            res = dot_f32(hv[e], wdb[lax.rem(i0 + u, slots)]).astype(BF16)
            etile[pl.ds(e * n_et, n_et)] = res.reshape(n_et, TILE, cw)

    def combine(n, g):
        b = lax.rem(n, 2)
        for u in range(per_src):
            s = g * per_src + u
            for t in range(n_st):
                esrc[u, t * TILE : (t + 1) * TILE, :] = etile[back_ref[0, s * 64 + t]]
        for u in range(per_src):
            s = g * per_src + u
            res = dot_f32(weigh[s], esrc[u])
            res = res[:tok] + (res[tok : 2 * tok] + res[2 * tok :])
            for hf in range(2):
                part[b, hf, s // 4, pl.ds(pl.multiple_of(lax.rem(s, 4) * tok, tok), tok), :] = res[:, hf * hw : (hf + 1) * hw]

    def shared_up(i):
        ahead = i + wsb.shape[0] - 1

        @pl.when(ahead < n_s)
        def _():
            start(ws_copies(ahead))

        wait(ws_copies(i))
        both = dot_f32(xn_ref[...], wsb[lax.rem(i, wsb.shape[0])])
        hs[i] = (jax.nn.silu(both[:, :sw]) * both[:, sw:]).astype(BF16)

    def step(s, carry):
        n, j = s // per_chunk, lax.rem(s, per_chunk)
        pl.when(j < n_down)(lambda: down(n, j))
        pl.when(j >= n_down)(lambda: combine(n, j - n_down))
        pl.when(j == per_chunk - 1)(lambda: d_copy(n).start())

        @pl.when(j == 1)
        def _():
            pl.when(n >= 1)(lambda: stage_p(n - 1))
            pl.when(n >= 4)(lambda: stage_f(n - 4))

        pl.when((j == n_down) & (n >= 2))(lambda: stage_q(n - 2))

        return carry

    lax.fori_loop(0, n_steps, step, 0)

    last = jnp.int32(n_chunk - 1)

    def up_step(i, carry):
        shared_up(i)
        pl.when(i == 1)(lambda: stage_p(last))
        pl.when(i == 4)(lambda: stage_q(last - 1))

        @pl.when(i == 8)
        def _():
            stage_f(last - 3)
            stage_f(last - 2)

        return carry

    lax.fori_loop(0, n_s, up_step, 0)
    for i in range(n_d):
        wds_copy(jnp.int32(i)).wait()
        res = jnp.zeros((tok, dw), F32)
        for k in range(n_s):
            res = res + dot_f32(hs[k], wdsb[i % 2, k * sw : (k + 1) * sw, :])
        out_ref[:, i * dw : (i + 1) * dw] = res.astype(BF16)
        if i + 2 < n_d:
            wds_copy(jnp.int32(i + 2)).start()
        if i == 1:
            stage_q(last)
    stage_f(last - 1)
    stage_f(last)
    for n in range(n_chunk):
        for hf in range(2):
            cols = slice(n * cw + hf * hw, n * cw + (hf + 1) * hw)
            out_ref[:, cols] = (hid_ref[:, cols].astype(F32) + out_ref[:, cols].astype(F32) + total[n, hf]).astype(BF16)


def solution(mesh):
    ep_size = mesh.shape["ep"]
    assert ep_size == 8

    def local_block(hidden_in, norm_gain, router_w, w_gate, w_up, w_down, ws_gate, ws_up, ws_down, expert_ids):
        tok, top_k = expert_ids.shape
        dim = hidden_in.shape[1]
        n_exp, _, inter = w_gate.shape
        s_inter = ws_gate.shape[1]
        cap = GROUPS * ((top_k + GROUP_LIMIT - 1) // GROUP_LIMIT) * tok // n_exp
        n_kc, slots = 4, 3
        kw = dim // n_kc
        pair_cap = cap * n_exp // ep_size
        n_st = (pair_cap + 14 * n_exp) // TILE + n_exp
        n_slot = -(-(n_st + 1) * TILE // 128) * 128
        n_st = n_slot // TILE
        assert n_st <= 64
        vmem = pl.BlockSpec(memory_space=pltpu.VMEM)
        smem = pl.BlockSpec(memory_space=pltpu.SMEM)
        hbm = pl.BlockSpec(memory_space=pl.ANY)
        dma = pltpu.SemaphoreType.DMA
        h, rg, xn, _, back = pl.pallas_call(
            functools.partial(gather_up_kernel, n_kc),
            out_shape=(
                jax.ShapeDtypeStruct((n_exp, cap, inter), BF16),
                jax.ShapeDtypeStruct((8, 2 * n_exp, 256), F32),
                jax.ShapeDtypeStruct((tok, dim), BF16),
                jax.ShapeDtypeStruct((n_exp, 256), jnp.int32),
                jax.ShapeDtypeStruct((1, 512), jnp.int32),
            ),
            in_specs=[vmem, vmem, vmem, vmem, hbm, hbm],
            out_specs=(hbm, vmem, hbm, hbm, vmem),
            scratch_shapes=[
                pltpu.VMEM((n_kc, 8 * tok, kw), BF16),
                pltpu.VMEM((8, n_slot, tok), BF16),
                pltpu.VMEM((7 * n_st + 64, TILE, kw), BF16),
                pltpu.VMEM((n_exp, cap, 2 * inter), F32),
                pltpu.VMEM((slots, kw, 2 * inter), BF16),
                pltpu.VMEM((2, cap, inter), BF16),
                pltpu.VMEM((2, cap, kw), BF16),
                pltpu.VMEM((8, n_exp, 256), F32),
                pltpu.VMEM((8, n_exp, 256), F32),
                pltpu.VMEM((8, 8, 256), jnp.int32),
                pltpu.VMEM((n_exp, 256), jnp.int32),
                pltpu.SMEM((n_exp, 256), jnp.int32),
                pltpu.VMEM((8, n_exp, 256), F32),
                pltpu.VMEM((8, n_exp, 256), F32),
                pltpu.VMEM((8, 256), jnp.int32),
                dma((slots, 2)),
                dma((2,)),
                dma((2,)),
                dma((n_kc,)),
                dma((8,)),
                dma((8,)),
                dma((8,)),
                dma((8,)),
                dma((n_kc, 9)),
                dma((n_kc, 9)),
            ],
            compiler_params=pltpu.CompilerParams(collective_id=0, has_side_effects=True, vmem_limit_bytes=VMEM_LIMIT),
            name="gather_up",
        )(hidden_in, norm_gain.reshape(1, dim), router_w, expert_ids.T, w_gate, w_up)

        n_chunk, dslots = 8, 8
        cw = dim // n_chunk
        hw = cw // 2
        sw, dw = 256, 512
        return pl.pallas_call(
            functools.partial(down_kernel, n_chunk),
            out_shape=jax.ShapeDtypeStruct((tok, dim), BF16),
            in_specs=[vmem, vmem, vmem, smem, hbm, hbm, hbm, hbm, hbm],
            out_specs=vmem,
            scratch_shapes=[
                pltpu.VMEM((n_exp, cap, inter), BF16),
                pltpu.VMEM((8, 3 * tok, n_slot), BF16),
                pltpu.VMEM((dslots, inter, cw), BF16),
                pltpu.VMEM((n_exp * cap // TILE, TILE, cw), BF16),
                pltpu.VMEM((4, n_slot, cw), BF16),
                pltpu.VMEM((2, 2, 2, 4 * tok, hw), F32),
                pltpu.VMEM((2, 2, 4 * tok, hw), F32),
                pltpu.VMEM((2, 2, 2, 2, tok, hw), F32),
                pltpu.VMEM((4, 2, 2, tok, hw), F32),
                pltpu.VMEM((4, 2, 2, tok, hw), F32),
                pltpu.VMEM((4, 2, tok, hw), F32),
                pltpu.VMEM((n_chunk, 2, tok, hw), F32),
                pltpu.VMEM((5, dim, 2 * sw), BF16),
                pltpu.VMEM((2, s_inter, dw), BF16),
                pltpu.VMEM((s_inter // sw, tok, sw), BF16),
                dma((n_exp,)),
                dma((dslots,)),
                dma((5, 2)),
                dma((2,)),
                dma((2,)),
                dma((2,)),
                dma((4, 2)),
                dma((4, 2)),
                dma((4, 2)),
                dma((4, 2)),
            ],
            compiler_params=pltpu.CompilerParams(collective_id=1, has_side_effects=True, vmem_limit_bytes=VMEM_LIMIT),
            name="down_sum",
        )(hidden_in, xn, rg, back, h, w_down, ws_gate, ws_up, ws_down)

    row_spec = P(("dp", "ep"), None)
    in_specs = (row_spec, P(), P(), P("ep"), P("ep"), P("ep"), P(), P(), P(), row_spec)
    return jax.shard_map(local_block, mesh=mesh, in_specs=in_specs, out_specs=row_spec, check_vma=False)
```

```python
import functools

import jax
import jax.numpy as jnp
from jax import lax
from jax.experimental import pallas as pl
from jax.experimental.pallas import tpu as pltpu
from jax.sharding import PartitionSpec as P

NORM_EPS = 1e-6
ROUTE_SCALE = 2.5
GROUPS = 8
GROUP_LIMIT = 4
F32 = jnp.float32
BF16 = jnp.bfloat16
VMEM_LIMIT = 67_000_000
TILE = 16


def dot_f32(a, b):
    return jnp.dot(a, b, preferred_element_type=F32)


def place():
    me = lax.axis_index("ep")
    core = lax.rem(me, 2)
    x = lax.rem(me // 2, 2)
    y = me // 4
    return me, core, x, y, me + 1 - 2 * core, me + 2 - 4 * x, me + 4 - 8 * y


def pos_of(dev):
    return lax.rem(dev, 2) * 4 + dev // 2


def rcopy(src, dst, ssem, rsem, dev):
    return pltpu.make_async_remote_copy(
        src_ref=src, dst_ref=dst, send_sem=ssem, recv_sem=rsem, device_id={"ep": dev}, device_id_type=pl.DeviceIdType.MESH
    )


def split3(v):
    hi = v.astype(BF16)
    rest = v - hi.astype(F32)
    mid = rest.astype(BF16)
    return hi, mid, (rest - mid.astype(F32)).astype(BF16)


def iota(shape, axis):
    return lax.broadcasted_iota(jnp.int32, shape, axis)


def gather_up_kernel(
    n_kc, hid_ref, gain_ref, rw_ref, ids_ref, wg_ref, wu_ref, h_ref, rg_ref, xn_ref, tab_ref, back_ref,
    xall, pick, xsrc, acc, wbuf, hbuf, xe, meta_s, meta_r, ids_r, tab_v, tab_s,
    cid, ids_t, w_sem, h_sem, t_sem, x_sem, i_send, i_recv, m_send, m_recv, a_send, a_recv,
):
    me, core, x, y, sib, xnb, ynb = place()
    tok, dim = hid_ref.shape
    n_exp, _, inter = wg_ref.shape
    cap = h_ref.shape[1]
    kw = dim // n_kc
    half = tok // 2
    n_steps = n_exp * n_kc
    slots = wbuf.shape[0]
    n_et = cap // TILE
    n_st = pick.shape[1] // TILE

    def w_copies(s):
        e, kc, slot = lax.rem(s, n_exp), s // n_exp, lax.rem(s, slots)
        rows = pl.ds(pl.multiple_of(kc * kw, kw), kw)
        return (
            pltpu.make_async_copy(wg_ref.at[e, rows, :], wbuf.at[slot, :, pl.ds(0, inter)], w_sem.at[slot, 0]),
            pltpu.make_async_copy(wu_ref.at[e, rows, :], wbuf.at[slot, :, pl.ds(inter, inter)], w_sem.at[slot, 1]),
        )

    def w_start(s):
        for c in w_copies(s):
            c.start()

    for s in range(slots - 1):
        w_start(jnp.int32(s))

    ids_t[...] = jnp.full(ids_t.shape, -1, jnp.int32)
    ids_t[: ids_ref.shape[0], :tok] = ids_ref[...]

    barrier = pltpu.get_barrier_semaphore()
    for k in range(1, 8):
        pl.semaphore_signal(barrier, inc=1, device_id={"ep": lax.rem(me + k, 8)}, device_id_type=pl.DeviceIdType.MESH)

    x_f32 = hid_ref[...].astype(F32)
    inv_rms = lax.rsqrt(jnp.mean(x_f32 * x_f32, axis=-1, keepdims=True) + NORM_EPS)
    x_norm = (x_f32 * inv_rms * gain_ref[...]).astype(BF16)
    my_pos = pos_of(me)
    my_rows = pl.ds(pl.multiple_of(my_pos * tok, tok), tok)
    for kc in range(n_kc):
        xall[kc, my_rows, :] = x_norm[:, kc * kw : (kc + 1) * kw]

    def xn_copy(kc):
        return pltpu.make_async_copy(xall.at[kc, my_rows, :], xn_ref.at[:, pl.ds(kc * kw, kw)], x_sem.at[kc])

    for kc in range(n_kc):
        xn_copy(kc).start()
    pl.semaphore_wait(barrier, 7)

    def block(kc, dev, part=None):
        start = pos_of(dev) * tok + (0 if part is None else part * half)
        n = tok if part is None else half
        return xall.at[kc, pl.ds(pl.multiple_of(start, half), n), :]

    def send(kc, kind, dev_src, to, part=None):
        ref = block(kc, dev_src, part)
        return rcopy(ref, ref, a_send.at[kc, kind], a_recv.at[kc, kind], to)

    diag = me + 6 - 4 * x - 8 * y
    kinds = (
        (me, sib, None), (me, xnb, 0), (me, ynb, 1), (xnb, ynb, 0), (ynb, xnb, 1),
        (xnb, sib, None), (ynb, sib, None), (diag, sib, 0), (diag, sib, 1), (me, xnb, 1), (me, ynb, 0),
    )

    def copy(kc, kind):
        src, to, part = kinds[kind]
        return send(kc, kind, src, to, part)

    def start(kc, which):
        for kind in which:
            copy(kc, kind).start()

    def received(kc, which):
        for kind in which:
            copy(kc, kind).wait_recv()

    def serve_a(kc):
        received(kc, (1, 2))
        start(kc, (3, 4))
        received(kc, (9, 10))
        start(kc, (5, 6))
        pl.when(kc + 1 < n_kc)(lambda: start(kc + 1, (1, 2, 9, 10, 0)))

    def serve_b(kc):
        received(kc, (3, 4))
        start(kc, (7, 8))

    def meta(k):
        to = lax.rem(me + k, 8)
        return rcopy(meta_s.at[to], meta_r.at[my_pos], m_send.at[k], m_recv.at[k], to)

    def ids_copy(k):
        return rcopy(ids_t, ids_r.at[my_pos], i_send.at[k], i_recv.at[k], lax.rem(me + k, 8))

    for k in range(1, 8):
        ids_copy(k).start()
    start(0, (1, 2, 9, 10, 0))
    ids_r[pl.ds(my_pos, 1)] = ids_t[...].reshape(1, 8, 256)

    parts = lax.dot_general(
        jnp.concatenate(split3(rw_ref[...]), axis=0), x_norm, (((1,), (1,)), ((), ())), preferred_element_type=F32
    )
    logits = parts[:64] + (parts[64:128] + parts[128:192])
    scores = jax.nn.sigmoid(logits)
    exp_iota = iota(scores.shape, 0)
    chosen = exp_iota == ids_t[0:1, :tok]
    for j in range(1, 6):
        chosen = chosen | (exp_iota == ids_t[j : j + 1, :tok])
    picked = jnp.where(chosen, scores, 0.0)
    gates = ROUTE_SCALE * picked / jnp.sum(picked, axis=0, keepdims=True)
    meta_s[...] = jnp.zeros(meta_s.shape, F32)
    for d in range(8):
        meta_s[d, :, 0:tok] = gates[d * n_exp : (d + 1) * n_exp, :]
    meta_r[pl.ds(my_pos, 1)] = meta_s[pl.ds(me, 1)]
    for k in range(1, 8):
        meta(k).start()
    for k in range(1, 8):
        ids_copy(k).wait_recv()

    my_exp = me * n_exp + iota((n_exp, 256), 0)
    masks = []
    for s in range(8):
        hit = my_exp == ids_r[s, 0:1, :]
        for j in range(1, 6):
            hit = hit | (my_exp == ids_r[s, j : j + 1, :])
        masks.append(hit)
    ones = jnp.concatenate([jnp.where(m, 1.0, 0.0) for m in masks], axis=0).astype(BF16)
    upper = iota((256, 256), 0) <= iota((256, 256), 1)
    cums = dot_f32(ones, jnp.where(upper, 1.0, 0.0).astype(BF16))
    cums = [cums[s * n_exp : (s + 1) * n_exp] for s in range(8)]

    lane = iota((n_exp, 128), 1)
    base = jnp.zeros((n_exp, 128), F32)
    count = jnp.zeros((n_exp, 128), F32)
    before = jnp.zeros((n_exp, 1), F32)
    for s in range(8):
        n = cums[s][:, 255:256]
        base = jnp.where(lane == s, before, base)
        count = jnp.where(lane == s, n, count)
        before = before + n
    base, count = base.astype(jnp.int32), count.astype(jnp.int32)
    first = base // TILE
    tiles = jnp.where(count > 0, (base + count - 1) // TILE - first + 1, 0)
    sub = iota((n_exp, 128), 0)
    ends = tiles
    for d in (1, 2, 4):
        ends = ends + jnp.where(sub >= d, pltpu.roll(ends, d, 0), 0)
    begin = ends - tiles
    shift = ((begin - first) * TILE + base).astype(F32)

    for s in range(8):
        slot_id = jnp.where(masks[s], cums[s] - 1.0 + shift[:, s : s + 1], -1.0)
        by_col = jnp.full((8, 256), -1.0, F32)
        for e in range(n_exp):
            by_col = jnp.where(ids_r[s] == me * n_exp + e, slot_id[e : e + 1], by_col)
        cid[s] = by_col

    rows24 = jnp.concatenate([first, tiles, begin], axis=0).astype(F32).astype(BF16)
    src = iota((128, 768), 0)
    col = iota((128, 768), 1)
    spread = jnp.where(jnp.where(col < 256, col % 8, (col - 256) // 64) == src, 1.0, 0.0).astype(BF16)
    table = dot_f32(rows24, spread).astype(jnp.int32)
    t_first, t_tiles, t_begin = table[:n_exp], table[n_exp : 2 * n_exp], table[2 * n_exp :]
    col = iota((n_exp, 256), 1)
    nth = col // 8 - t_first[:, :256]
    valid = (nth >= 0) & (nth < t_tiles[:, :256])
    tab_v[...] = jnp.where(valid, t_begin[:, :256] + nth, n_st - 1)
    out = pltpu.make_async_copy(tab_v, tab_ref, t_sem.at[0])
    out.start()
    nth = iota((n_exp, 512), 1) % 64 - t_begin[:, 256:]
    valid = (nth >= 0) & (nth < t_tiles[:, 256:])
    back = jnp.where(valid, iota((n_exp, 512), 0) * n_et + t_first[:, 256:] + nth, 0)
    back_ref[...] = jnp.sum(back, axis=0, keepdims=True)

    def build(s, carry):
        for q in range(0, n_st * TILE, 128):
            want = (iota((128, 256), 0) + q).astype(F32)
            got = want == cid[s, 0:1, :]
            for j in range(1, 6):
                got = got | (want == cid[s, j : j + 1, :])
            pick[s, q : q + 128, :] = jnp.where(got, 1.0, 0.0).astype(BF16)[:, :tok]
        return carry

    lax.fori_loop(0, 4, build, 0)
    out.wait()
    load = pltpu.make_async_copy(tab_ref, tab_s, t_sem.at[1])
    load.start()
    serve_a(0)
    lax.fori_loop(4, 8, build, 0)
    load.wait()

    def select(kc):
        received(kc, (0, 5, 6, 7, 8))

        for s in range(8):
            for n in range(0, kw, 256):
                res = dot_f32(pick[s], xall[kc, s * tok : (s + 1) * tok, n : n + 256]).astype(BF16)
                xsrc[s * n_st : (s + 1) * n_st, :, n : n + 256] = res.reshape(n_st, TILE, 256)

    def fill(s):
        e, slot = lax.rem(s, n_exp), lax.rem(s, 2)
        for t in range(n_et):
            got = [xsrc[k * n_st + (tab_s[e, t * 8 + k] & 63)] for k in range(8)]
            while len(got) > 1:
                got = [got[i] + got[i + 1] for i in range(0, len(got), 2)]
            xe[slot, t * TILE : (t + 1) * TILE, :] = got[0]

    serve_b(0)
    select(0)
    fill(jnp.int32(0))

    def step(s, carry):
        e, kc = lax.rem(s, n_exp), s // n_exp
        slot = lax.rem(s, slots)
        more = kc + 1 < n_kc
        pl.when(more & (e == 2))(lambda: serve_a(kc + 1))
        pl.when(more & (e == 5))(lambda: serve_b(kc + 1))
        pl.when(more & (e == n_exp - 1))(lambda: select(kc + 1))

        @pl.when(s + slots - 1 < n_steps)
        def _():
            w_start(s + slots - 1)

        for c in w_copies(s):
            c.wait()
        rows = xe.at[lax.rem(s, 2)]

        @pl.when(kc < n_kc - 1)
        def _():
            fill(s + 1)
            for n in range(0, 2 * inter, 256):
                part = dot_f32(rows[...], wbuf[slot, :, n : n + 256])
                acc[e, :, n : n + 256] = jnp.where(kc > 0, acc[e, :, n : n + 256], 0.0) + part

        @pl.when(kc == n_kc - 1)
        def _():
            b = lax.rem(e, 2)

            @pl.when(e >= 2)
            def _():
                pltpu.make_async_copy(hbuf.at[b], h_ref.at[e - 2], h_sem.at[b]).wait()

            fill(s + 1)
            for n in range(0, inter, 256):
                w = min(256, inter - n)
                g = acc[e, :, n : n + w] + dot_f32(rows[...], wbuf[slot, :, n : n + w])
                u = acc[e, :, inter + n : inter + n + w] + dot_f32(rows[...], wbuf[slot, :, inter + n : inter + n + w])
                hbuf[b, :, n : n + w] = (jax.nn.silu(g) * u).astype(BF16)
            pltpu.make_async_copy(hbuf.at[b], h_ref.at[e], h_sem.at[b]).start()

        return carry

    lax.fori_loop(0, n_steps, step, 0)

    for e in range(n_exp - 2, n_exp):
        pltpu.make_async_copy(hbuf.at[e % 2], h_ref.at[e], h_sem.at[e % 2]).wait()
    for k in range(1, 8):
        meta(k).wait_recv()
    for s in range(8):
        gate_by_col = jnp.zeros((8, 256), F32)
        for e in range(n_exp):
            gate_by_col = jnp.where(ids_r[s] == me * n_exp + e, meta_r[s, e : e + 1, :], gate_by_col)
        rg_ref[s, :8] = cid[s]
        rg_ref[s, 8:] = gate_by_col
    for kc in range(n_kc):
        xn_copy(kc).wait()
    for k in range(1, 8):
        ids_copy(k).wait_send()
        meta(k).wait_send()
    for kc in range(n_kc):
        for kind in range(len(kinds)):
            copy(kc, kind).wait_send()


def down_kernel(
    n_chunk, rg_ref, back_ref, hid_hbm, xn_hbm, h_ref, wd_ref, wsg_ref, wsu_ref, wsd_ref, out_ref,
    hv, weigh, wdb, etile, esrc, part, got0, mid, got1, quart, got2, total, wsb, wdsb, hs, xn_ref, hid_ref, x_sem,
    hv_sem, wd_sem, ws_sem, wds_sem, d_send, d_recv, p_send, p_recv, q_send, q_recv,
):
    me, core, x, y, sib, xnb, ynb = place()
    n_exp, cap, inter = h_ref.shape
    tok, dim = xn_hbm.shape
    n_et = cap // TILE
    n_slot = weigh.shape[-1]
    n_st = n_slot // TILE
    cw = dim // n_chunk
    hw = cw // 2
    unroll = 2
    n_down = n_exp // unroll
    per_src = 4
    per_chunk = n_down + 8 // per_src
    n_steps = n_chunk * per_chunk
    slots = wdb.shape[0]
    sw = wsb.shape[-1] // 2
    n_s = wsg_ref.shape[1] // sw
    dw = wdsb.shape[-1]
    n_d = dim // dw

    def wd_copy(i):
        e, n, slot = lax.rem(i, n_exp), i // n_exp, lax.rem(i, slots)
        return pltpu.make_async_copy(wd_ref.at[e, :, pl.ds(pl.multiple_of(n * cw, cw), cw)], wdb.at[slot], wd_sem.at[slot])

    def h_copy(e):
        return pltpu.make_async_copy(h_ref.at[e], hv.at[e], hv_sem.at[e])

    def ws_copies(i):
        cols = pl.ds(pl.multiple_of(i * sw, sw), sw)
        slot = lax.rem(i, wsb.shape[0])
        return (
            pltpu.make_async_copy(wsg_ref.at[:, cols], wsb.at[slot, :, pl.ds(0, sw)], ws_sem.at[slot, 0]),
            pltpu.make_async_copy(wsu_ref.at[:, cols], wsb.at[slot, :, pl.ds(sw, sw)], ws_sem.at[slot, 1]),
        )

    def wds_copy(i):
        slot = lax.rem(i, 2)
        return pltpu.make_async_copy(wsd_ref.at[:, pl.ds(pl.multiple_of(i * dw, dw), dw)], wdsb.at[slot], wds_sem.at[slot])

    def start(copies):
        for c in copies:
            c.start()

    def wait(copies):
        for c in copies:
            c.wait()

    h_copy(0).start()
    for i in range(slots - unroll):
        wd_copy(jnp.int32(i)).start()
    for e in range(1, n_exp):
        h_copy(e).start()
    for i in range(wsb.shape[0] - 1):
        start(ws_copies(jnp.int32(i)))
    for i in range(2):
        wds_copy(jnp.int32(i)).start()
    pltpu.make_async_copy(xn_hbm, xn_ref, x_sem.at[0]).start()
    pltpu.make_async_copy(hid_hbm, hid_ref, x_sem.at[1]).start()

    barrier = pltpu.get_barrier_semaphore()
    for dev in (sib, xnb, ynb):
        pl.semaphore_signal(barrier, inc=1, device_id={"ep": dev}, device_id_type=pl.DeviceIdType.MESH)

    def build(s):
        slot = iota((tok, n_slot), 1).astype(F32)
        val = jnp.zeros((tok, n_slot), F32)
        cols = jnp.concatenate([rg_ref[s], jnp.zeros((112, 256), F32)], axis=0).T[:tok]
        for k in range(6):
            val = jnp.where(cols[:, k : k + 1] == slot, cols[:, 8 + k : 9 + k], val)
        for k, piece in enumerate(split3(val)):
            weigh[s, k * tok : (k + 1) * tok, :] = piece

    def d_copy(n):
        b = lax.rem(n, 2)
        return rcopy(part.at[b, :, 1 - core], got0.at[b], d_send.at[b], d_recv.at[b], sib)

    def p_copies(n):
        b = lax.rem(n, 4)
        return (
            rcopy(mid.at[lax.rem(n, 2), 0, :, 1 - x], got1.at[b, 0], p_send.at[b, 0], p_recv.at[b, 0], xnb),
            rcopy(mid.at[lax.rem(n, 2), 1, 1 - y], got1.at[b, 1], p_send.at[b, 1], p_recv.at[b, 1], ynb),
        )

    def q_copies(n):
        b = lax.rem(n, 4)
        return (
            rcopy(quart.at[b, 0, 1 - y], got2.at[b, 0], q_send.at[b, 0], q_recv.at[b, 0], ynb),
            rcopy(quart.at[b, 1, 1 - x], got2.at[b, 1], q_send.at[b, 1], q_recv.at[b, 1], xnb),
        )

    def stage_p(n):
        b = lax.rem(n, 2)
        d_copy(n).wait()
        for hf in range(2):
            for yy in range(2):
                for xx in range(2):
                    rows = pl.ds((yy * 2 + xx) * tok, tok)
                    mid[b, hf, yy, xx] = part[b, hf, core, rows, :] + got0[b, hf, rows, :]
        start(p_copies(n))

    def stage_q(n):
        b = lax.rem(n, 4)
        wait(p_copies(n))
        for k in range(2):
            quart[b, 0, k] = mid[lax.rem(n, 2), 0, k, x] + got1[b, 0, k]
            quart[b, 1, k] = mid[lax.rem(n, 2), 1, y, k] + got1[b, 1, k]
        start(q_copies(n))

    def stage_f(n):
        b = lax.rem(n, 4)
        wait(q_copies(n))
        total[n, 0] = quart[b, 0, y] + got2[b, 0]
        total[n, 1] = quart[b, 1, x] + got2[b, 1]

    def down(n, j):
        i0 = n * n_exp + j * unroll
        for u in range(unroll):
            i = i0 + slots - unroll + u

            @pl.when(i < n_chunk * n_exp)
            def _():
                wd_copy(i).start()

        for u in range(unroll):
            wd_copy(i0 + u).wait()

        def products():
            for u in range(unroll):
                e = j * unroll + u
                res = dot_f32(hv[e], wdb[lax.rem(i0 + u, slots)]).astype(BF16)
                etile[pl.ds(e * n_et, n_et)] = res.reshape(n_et, TILE, cw)

        @pl.when(n == 0)
        def _():
            for u in range(unroll):
                h_copy(j * unroll + u).wait()
            products()
            for u in range(8 // n_down):
                build(j * (8 // n_down) + u)

        pl.when(n > 0)(products)

    def combine(n, g):
        b = lax.rem(n, 2)
        for u in range(per_src):
            s = (g + 1 - core - 2 * g * (1 - core)) * per_src + u
            for t in range(n_st):
                esrc[u, t * TILE : (t + 1) * TILE, :] = etile[back_ref[0, s * 64 + t]]
        for u in range(per_src):
            s = (g + 1 - core - 2 * g * (1 - core)) * per_src + u
            res = dot_f32(weigh[s], esrc[u])
            res = res[:tok] + (res[tok : 2 * tok] + res[2 * tok :])
            for hf in range(2):
                part[b, hf, s // 4, u * tok : (u + 1) * tok, :] = res[:, hf * hw : (hf + 1) * hw]

    def shared_up(i):
        ahead = i + wsb.shape[0] - 1

        @pl.when(ahead < n_s)
        def _():
            start(ws_copies(ahead))

        wait(ws_copies(i))
        both = dot_f32(xn_ref[...], wsb[lax.rem(i, wsb.shape[0])])
        hs[i] = (jax.nn.silu(both[:, :sw]) * both[:, sw:]).astype(BF16)

    def step(s, carry):
        n, j = s // per_chunk, lax.rem(s, per_chunk)
        pl.when(j < n_down)(lambda: down(n, j))
        pl.when(j >= n_down)(lambda: combine(n, j - n_down))
        @pl.when(j == n_down)
        def _():
            pl.when(n == 0)(lambda: pl.semaphore_wait(barrier, 3))
            d_copy(n).start()

        @pl.when(j == 0)
        def _():
            pl.when(n >= 1)(lambda: stage_p(n - 1))
            pl.when(n >= 4)(lambda: stage_f(n - 4))

        pl.when((j == n_down) & (n >= 2))(lambda: stage_q(n - 2))

        return carry

    lax.fori_loop(0, n_steps, step, 0)

    last = jnp.int32(n_chunk - 1)

    def up_step(i, carry):
        shared_up(i)
        pl.when(i == 0)(lambda: stage_p(last))
        pl.when(i == 4)(lambda: stage_q(last - 1))

        @pl.when(i == 8)
        def _():
            stage_f(last - 3)
            stage_f(last - 2)

        return carry

    pltpu.make_async_copy(xn_hbm, xn_ref, x_sem.at[0]).wait()
    pltpu.make_async_copy(hid_hbm, hid_ref, x_sem.at[1]).wait()
    lax.fori_loop(0, n_s, up_step, 0)
    for i in range(n_d):
        wds_copy(jnp.int32(i)).wait()
        res = jnp.zeros((tok, dw), F32)
        for k in range(n_s):
            res = res + dot_f32(hs[k], wdsb[i % 2, k * sw : (k + 1) * sw, :])
        out_ref[:, i * dw : (i + 1) * dw] = res.astype(BF16)
        if i + 2 < n_d:
            wds_copy(jnp.int32(i + 2)).start()
        if i == 1:
            stage_q(last)
    stage_f(last - 1)
    stage_f(last)
    for n in range(n_chunk):
        for hf in range(2):
            cols = slice(n * cw + hf * hw, n * cw + (hf + 1) * hw)
            out_ref[:, cols] = (hid_ref[:, cols].astype(F32) + out_ref[:, cols].astype(F32) + total[n, hf]).astype(BF16)


def solution(mesh):
    ep_size = mesh.shape["ep"]
    assert ep_size == 8

    def local_block(hidden_in, norm_gain, router_w, w_gate, w_up, w_down, ws_gate, ws_up, ws_down, expert_ids):
        tok, top_k = expert_ids.shape
        dim = hidden_in.shape[1]
        n_exp, _, inter = w_gate.shape
        s_inter = ws_gate.shape[1]
        cap = GROUPS * ((top_k + GROUP_LIMIT - 1) // GROUP_LIMIT) * tok // n_exp
        n_kc, slots = 4, 3
        kw = dim // n_kc
        pair_cap = cap * n_exp // ep_size
        n_st = (pair_cap + 14 * n_exp) // TILE + n_exp
        n_slot = -(-(n_st + 1) * TILE // 128) * 128
        n_st = n_slot // TILE
        assert n_st <= 64
        vmem = pl.BlockSpec(memory_space=pltpu.VMEM)
        smem = pl.BlockSpec(memory_space=pltpu.SMEM)
        hbm = pl.BlockSpec(memory_space=pl.ANY)
        dma = pltpu.SemaphoreType.DMA
        h, rg, xn, _, back = pl.pallas_call(
            functools.partial(gather_up_kernel, n_kc),
            out_shape=(
                jax.ShapeDtypeStruct((n_exp, cap, inter), BF16),
                jax.ShapeDtypeStruct((8, 16, 256), F32),
                jax.ShapeDtypeStruct((tok, dim), BF16),
                jax.ShapeDtypeStruct((n_exp, 256), jnp.int32),
                jax.ShapeDtypeStruct((1, 512), jnp.int32),
            ),
            in_specs=[vmem, vmem, vmem, vmem, hbm, hbm],
            out_specs=(hbm, vmem, hbm, hbm, vmem),
            scratch_shapes=[
                pltpu.VMEM((n_kc, 8 * tok, kw), BF16),
                pltpu.VMEM((8, n_slot, tok), BF16),
                pltpu.VMEM((7 * n_st + 64, TILE, kw), BF16),
                pltpu.VMEM((n_exp, cap, 2 * inter), F32),
                pltpu.VMEM((slots, kw, 2 * inter), BF16),
                pltpu.VMEM((2, cap, inter), BF16),
                pltpu.VMEM((2, cap, kw), BF16),
                pltpu.VMEM((8, n_exp, 256), F32),
                pltpu.VMEM((8, n_exp, 256), F32),
                pltpu.VMEM((8, 8, 256), jnp.int32),
                pltpu.VMEM((n_exp, 256), jnp.int32),
                pltpu.SMEM((n_exp, 256), jnp.int32),
                pltpu.VMEM((8, 8, 256), F32),
                pltpu.VMEM((8, 256), jnp.int32),
                dma((slots, 2)),
                dma((2,)),
                dma((2,)),
                dma((n_kc,)),
                dma((8,)),
                dma((8,)),
                dma((8,)),
                dma((8,)),
                dma((n_kc, 11)),
                dma((n_kc, 11)),
            ],
            compiler_params=pltpu.CompilerParams(collective_id=0, has_side_effects=True, vmem_limit_bytes=VMEM_LIMIT),
            name="gather_up",
        )(hidden_in, norm_gain.reshape(1, dim), router_w, expert_ids.T, w_gate, w_up)

        n_chunk, dslots = 8, 12
        cw = dim // n_chunk
        hw = cw // 2
        sw, dw = 256, 512
        return pl.pallas_call(
            functools.partial(down_kernel, n_chunk),
            out_shape=jax.ShapeDtypeStruct((tok, dim), BF16),
            in_specs=[vmem, smem, hbm, hbm, hbm, hbm, hbm, hbm, hbm],
            out_specs=vmem,
            scratch_shapes=[
                pltpu.VMEM((n_exp, cap, inter), BF16),
                pltpu.VMEM((8, 3 * tok, n_slot), BF16),
                pltpu.VMEM((dslots, inter, cw), BF16),
                pltpu.VMEM((n_exp * cap // TILE, TILE, cw), BF16),
                pltpu.VMEM((4, n_slot, cw), BF16),
                pltpu.VMEM((2, 2, 2, 4 * tok, hw), F32),
                pltpu.VMEM((2, 2, 4 * tok, hw), F32),
                pltpu.VMEM((2, 2, 2, 2, tok, hw), F32),
                pltpu.VMEM((4, 2, 2, tok, hw), F32),
                pltpu.VMEM((4, 2, 2, tok, hw), F32),
                pltpu.VMEM((4, 2, tok, hw), F32),
                pltpu.VMEM((n_chunk, 2, tok, hw), F32),
                pltpu.VMEM((5, dim, 2 * sw), BF16),
                pltpu.VMEM((2, s_inter, dw), BF16),
                pltpu.VMEM((s_inter // sw, tok, sw), BF16),
                pltpu.VMEM((tok, dim), BF16),
                pltpu.VMEM((tok, dim), BF16),
                dma((2,)),
                dma((n_exp,)),
                dma((dslots,)),
                dma((5, 2)),
                dma((2,)),
                dma((2,)),
                dma((2,)),
                dma((4, 2)),
                dma((4, 2)),
                dma((4, 2)),
                dma((4, 2)),
            ],
            compiler_params=pltpu.CompilerParams(collective_id=1, has_side_effects=True, vmem_limit_bytes=VMEM_LIMIT),
            name="down_sum",
        )(rg, back, hidden_in, xn, h, w_down, ws_gate, ws_up, ws_down)

    row_spec = P(("dp", "ep"), None)
    in_specs = (row_spec, P(), P(), P("ep"), P("ep"), P("ep"), P(), P(), P(), row_spec)
    return jax.shard_map(local_block, mesh=mesh, in_specs=in_specs, out_specs=row_spec, check_vma=False)
```

```python
import functools

import jax
import jax.numpy as jnp
from jax import lax
from jax.experimental import pallas as pl
from jax.experimental.pallas import tpu as pltpu
from jax.sharding import PartitionSpec as P

NORM_EPS = 1e-6
ROUTE_SCALE = 2.5
GROUPS = 8
GROUP_LIMIT = 4
F32 = jnp.float32
BF16 = jnp.bfloat16
VMEM_LIMIT = 67_000_000
TILE = 16


def dot_f32(a, b):
    return jnp.dot(a, b, preferred_element_type=F32)


def place():
    me = lax.axis_index("ep")
    core = lax.rem(me, 2)
    x = lax.rem(me // 2, 2)
    y = me // 4
    return me, core, x, y, me + 1 - 2 * core, me + 2 - 4 * x, me + 4 - 8 * y


def pos_of(dev):
    return lax.rem(dev, 2) * 4 + dev // 2


def rcopy(src, dst, ssem, rsem, dev):
    return pltpu.make_async_remote_copy(
        src_ref=src, dst_ref=dst, send_sem=ssem, recv_sem=rsem, device_id={"ep": dev}, device_id_type=pl.DeviceIdType.MESH
    )


def split3(v):
    hi = v.astype(BF16)
    rest = v - hi.astype(F32)
    mid = rest.astype(BF16)
    return hi, mid, (rest - mid.astype(F32)).astype(BF16)


def iota(shape, axis):
    return lax.broadcasted_iota(jnp.int32, shape, axis)


def gather_up_kernel(
    n_kc, hid_ref, gain_ref, rw_ref, ids_ref, wg_ref, wu_ref, h_ref, rg_ref, xn_ref, tab_ref, back_ref,
    xall, pick, xsrc, acc, wbuf, hbuf, xe, meta_s, meta_r, ids_r, tab_v, tab_s,
    cid, ids_t, w_sem, h_sem, t_sem, x_sem, i_send, i_recv, m_send, m_recv, a_send, a_recv,
):
    me, core, x, y, sib, xnb, ynb = place()
    tok, dim = hid_ref.shape
    n_exp, _, inter = wg_ref.shape
    cap = h_ref.shape[1]
    kw = dim // n_kc
    half = tok // 2
    n_steps = n_exp * n_kc
    slots = wbuf.shape[0]
    n_et = cap // TILE
    n_st = pick.shape[1] // TILE

    def w_copies(s):
        e, kc, slot = lax.rem(s, n_exp), s // n_exp, lax.rem(s, slots)
        rows = pl.ds(pl.multiple_of(kc * kw, kw), kw)
        return (
            pltpu.make_async_copy(wg_ref.at[e, rows, :], wbuf.at[slot, :, pl.ds(0, inter)], w_sem.at[slot, 0]),
            pltpu.make_async_copy(wu_ref.at[e, rows, :], wbuf.at[slot, :, pl.ds(inter, inter)], w_sem.at[slot, 1]),
        )

    def w_start(s):
        for c in w_copies(s):
            c.start()

    for s in range(slots - 1):
        w_start(jnp.int32(s))

    ids_t[...] = jnp.full(ids_t.shape, -1, jnp.int32)
    ids_t[: ids_ref.shape[0], :tok] = ids_ref[...]

    barrier = pltpu.get_barrier_semaphore()
    for k in range(1, 8):
        pl.semaphore_signal(barrier, inc=1, device_id={"ep": lax.rem(me + k, 8)}, device_id_type=pl.DeviceIdType.MESH)

    x_f32 = hid_ref[...].astype(F32)
    inv_rms = lax.rsqrt(jnp.mean(x_f32 * x_f32, axis=-1, keepdims=True) + NORM_EPS)
    x_norm = (x_f32 * inv_rms * gain_ref[...]).astype(BF16)
    my_pos = pos_of(me)
    my_rows = pl.ds(pl.multiple_of(my_pos * tok, tok), tok)
    for kc in range(n_kc):
        xall[kc, my_rows, :] = x_norm[:, kc * kw : (kc + 1) * kw]

    def xn_copy(kc):
        return pltpu.make_async_copy(xall.at[kc, my_rows, :], xn_ref.at[:, pl.ds(kc * kw, kw)], x_sem.at[kc])

    for kc in range(n_kc):
        xn_copy(kc).start()
    pl.semaphore_wait(barrier, 7)

    def block(kc, dev, part=None):
        start = pos_of(dev) * tok + (0 if part is None else part * half)
        n = tok if part is None else half
        return xall.at[kc, pl.ds(pl.multiple_of(start, half), n), :]

    def send(kc, kind, dev_src, to, part=None):
        ref = block(kc, dev_src, part)
        return rcopy(ref, ref, a_send.at[kc, kind], a_recv.at[kc, kind], to)

    diag = me + 6 - 4 * x - 8 * y
    kinds = (
        (me, sib, None), (me, xnb, 0), (me, ynb, 1), (xnb, ynb, 0), (ynb, xnb, 1),
        (xnb, sib, None), (ynb, sib, None), (diag, sib, 0), (diag, sib, 1), (me, xnb, 1), (me, ynb, 0),
    )

    def copy(kc, kind):
        src, to, part = kinds[kind]
        return send(kc, kind, src, to, part)

    def start(kc, which):
        for kind in which:
            copy(kc, kind).start()

    def received(kc, which):
        for kind in which:
            copy(kc, kind).wait_recv()

    def serve_a(kc):
        received(kc, (1, 2))
        start(kc, (3, 4))
        received(kc, (9, 10))
        start(kc, (5, 6))
        pl.when(kc + 1 < n_kc)(lambda: start(kc + 1, (1, 2, 9, 10, 0)))

    def serve_b(kc):
        received(kc, (3, 4))
        start(kc, (7, 8))

    def meta(k):
        to = lax.rem(me + k, 8)
        return rcopy(meta_s.at[to], meta_r.at[my_pos], m_send.at[k], m_recv.at[k], to)

    def ids_copy(k):
        return rcopy(ids_t, ids_r.at[my_pos], i_send.at[k], i_recv.at[k], lax.rem(me + k, 8))

    for k in range(1, 8):
        ids_copy(k).start()
    start(0, (1, 2, 9, 10, 0))
    ids_r[pl.ds(my_pos, 1)] = ids_t[...].reshape(1, 8, 256)

    parts = lax.dot_general(
        jnp.concatenate(split3(rw_ref[...]), axis=0), x_norm, (((1,), (1,)), ((), ())), preferred_element_type=F32
    )
    logits = parts[:64] + (parts[64:128] + parts[128:192])
    scores = jax.nn.sigmoid(logits)
    exp_iota = iota(scores.shape, 0)
    chosen = exp_iota == ids_t[0:1, :tok]
    for j in range(1, 6):
        chosen = chosen | (exp_iota == ids_t[j : j + 1, :tok])
    picked = jnp.where(chosen, scores, 0.0)
    gates = ROUTE_SCALE * picked / jnp.sum(picked, axis=0, keepdims=True)
    meta_s[...] = jnp.zeros(meta_s.shape, F32)
    for d in range(8):
        meta_s[d, :, 0:tok] = gates[d * n_exp : (d + 1) * n_exp, :]
    meta_r[pl.ds(my_pos, 1)] = meta_s[pl.ds(me, 1)]
    for k in range(1, 8):
        meta(k).start()
    for k in range(1, 8):
        ids_copy(k).wait_recv()

    my_exp = me * n_exp + iota((n_exp, 256), 0)
    masks = []
    for s in range(8):
        hit = my_exp == ids_r[s, 0:1, :]
        for j in range(1, 6):
            hit = hit | (my_exp == ids_r[s, j : j + 1, :])
        masks.append(hit)
    ones = jnp.concatenate([jnp.where(m, 1.0, 0.0) for m in masks], axis=0).astype(BF16)
    upper = iota((256, 256), 0) <= iota((256, 256), 1)
    cums = dot_f32(ones, jnp.where(upper, 1.0, 0.0).astype(BF16))
    cums = [cums[s * n_exp : (s + 1) * n_exp] for s in range(8)]

    lane = iota((n_exp, 128), 1)
    base = jnp.zeros((n_exp, 128), F32)
    count = jnp.zeros((n_exp, 128), F32)
    before = jnp.zeros((n_exp, 1), F32)
    for s in range(8):
        n = cums[s][:, 255:256]
        base = jnp.where(lane == s, before, base)
        count = jnp.where(lane == s, n, count)
        before = before + n
    base, count = base.astype(jnp.int32), count.astype(jnp.int32)
    first = base // TILE
    tiles = jnp.where(count > 0, (base + count - 1) // TILE - first + 1, 0)
    sub = iota((n_exp, 128), 0)
    ends = tiles
    for d in (1, 2, 4):
        ends = ends + jnp.where(sub >= d, pltpu.roll(ends, d, 0), 0)
    begin = ends - tiles
    shift = ((begin - first) * TILE + base).astype(F32)

    for s in range(8):
        slot_id = jnp.where(masks[s], cums[s] - 1.0 + shift[:, s : s + 1], -1.0)
        by_col = jnp.full((8, 256), -1.0, F32)
        for e in range(n_exp):
            by_col = jnp.where(ids_r[s] == me * n_exp + e, slot_id[e : e + 1], by_col)
        cid[s] = by_col

    rows24 = jnp.concatenate([first, tiles, begin], axis=0).astype(F32).astype(BF16)
    src = iota((128, 768), 0)
    col = iota((128, 768), 1)
    spread = jnp.where(jnp.where(col < 256, col % 8, (col - 256) // 64) == src, 1.0, 0.0).astype(BF16)
    table = dot_f32(rows24, spread).astype(jnp.int32)
    t_first, t_tiles, t_begin = table[:n_exp], table[n_exp : 2 * n_exp], table[2 * n_exp :]
    col = iota((n_exp, 256), 1)
    nth = col // 8 - t_first[:, :256]
    valid = (nth >= 0) & (nth < t_tiles[:, :256])
    tab_v[...] = jnp.where(valid, t_begin[:, :256] + nth, n_st - 1)
    out = pltpu.make_async_copy(tab_v, tab_ref, t_sem.at[0])
    out.start()
    nth = iota((n_exp, 512), 1) % 64 - t_begin[:, 256:]
    valid = (nth >= 0) & (nth < t_tiles[:, 256:])
    back = jnp.where(valid, iota((n_exp, 512), 0) * n_et + t_first[:, 256:] + nth, 0)
    back_ref[...] = jnp.sum(back, axis=0, keepdims=True)

    def build(s, carry):
        for q in range(0, n_st * TILE, 128):
            want = (iota((128, 256), 0) + q).astype(F32)
            got = want == cid[s, 0:1, :]
            for j in range(1, 6):
                got = got | (want == cid[s, j : j + 1, :])
            pick[s, q : q + 128, :] = jnp.where(got, 1.0, 0.0).astype(BF16)[:, :tok]
        return carry

    lax.fori_loop(0, 4, build, 0)
    out.wait()
    load = pltpu.make_async_copy(tab_ref, tab_s, t_sem.at[1])
    load.start()
    serve_a(0)
    lax.fori_loop(4, 8, build, 0)
    load.wait()

    def select(kc):
        received(kc, (0, 5, 6, 7, 8))

        for s in range(8):
            for n in range(0, kw, 256):
                res = dot_f32(pick[s], xall[kc, s * tok : (s + 1) * tok, n : n + 256]).astype(BF16)
                xsrc[s * n_st : (s + 1) * n_st, :, n : n + 256] = res.reshape(n_st, TILE, 256)

    def fill(s):
        e, slot = lax.rem(s, n_exp), lax.rem(s, 2)
        for t in range(n_et):
            got = [xsrc[k * n_st + (tab_s[e, t * 8 + k] & 63)] for k in range(8)]
            while len(got) > 1:
                got = [got[i] + got[i + 1] for i in range(0, len(got), 2)]
            xe[slot, t * TILE : (t + 1) * TILE, :] = got[0]

    serve_b(0)
    select(0)
    fill(jnp.int32(0))

    def step(s, carry):
        e, kc = lax.rem(s, n_exp), s // n_exp
        slot = lax.rem(s, slots)
        more = kc + 1 < n_kc
        pl.when(more & (e == 2))(lambda: serve_a(kc + 1))
        pl.when(more & (e == 5))(lambda: serve_b(kc + 1))
        pl.when(more & (e == n_exp - 1))(lambda: select(kc + 1))

        @pl.when(s + slots - 1 < n_steps)
        def _():
            w_start(s + slots - 1)

        for c in w_copies(s):
            c.wait()
        rows = xe.at[lax.rem(s, 2)]

        @pl.when(kc < n_kc - 1)
        def _():
            fill(s + 1)
            for n in range(0, 2 * inter, 256):
                part = dot_f32(rows[...], wbuf[slot, :, n : n + 256])
                acc[e, :, n : n + 256] = jnp.where(kc > 0, acc[e, :, n : n + 256], 0.0) + part

        @pl.when(kc == n_kc - 1)
        def _():
            b = lax.rem(e, 2)

            @pl.when(e >= 2)
            def _():
                pltpu.make_async_copy(hbuf.at[b], h_ref.at[e - 2], h_sem.at[b]).wait()

            fill(s + 1)
            for n in range(0, inter, 256):
                w = min(256, inter - n)
                g = acc[e, :, n : n + w] + dot_f32(rows[...], wbuf[slot, :, n : n + w])
                u = acc[e, :, inter + n : inter + n + w] + dot_f32(rows[...], wbuf[slot, :, inter + n : inter + n + w])
                hbuf[b, :, n : n + w] = (jax.nn.silu(g) * u).astype(BF16)
            pltpu.make_async_copy(hbuf.at[b], h_ref.at[e], h_sem.at[b]).start()

        return carry

    lax.fori_loop(0, n_steps, step, 0)

    for e in range(n_exp - 2, n_exp):
        pltpu.make_async_copy(hbuf.at[e % 2], h_ref.at[e], h_sem.at[e % 2]).wait()
    for k in range(1, 8):
        meta(k).wait_recv()
    for s in range(8):
        gate_by_col = jnp.zeros((8, 256), F32)
        for e in range(n_exp):
            gate_by_col = jnp.where(ids_r[s] == me * n_exp + e, meta_r[s, e : e + 1, :], gate_by_col)
        rg_ref[s, :8] = cid[s]
        rg_ref[s, 8:] = gate_by_col
    for kc in range(n_kc):
        xn_copy(kc).wait()
    for k in range(1, 8):
        ids_copy(k).wait_send()
        meta(k).wait_send()
    for kc in range(n_kc):
        for kind in range(len(kinds)):
            copy(kc, kind).wait_send()


def down_kernel(
    n_chunk, rg_ref, back_ref, hid_hbm, xn_hbm, h_ref, wd_ref, wsg_ref, wsu_ref, wsd_ref, out_ref,
    hv, weigh, wdb, etile, esrc, part, got0, mid, got1, quart, got2, total, wsb, wdsb, hs, xn_ref, hid_ref, x_sem,
    hv_sem, wd_sem, ws_sem, wds_sem, d_send, d_recv, p_send, p_recv, q_send, q_recv,
):
    me, core, x, y, sib, xnb, ynb = place()
    n_exp, cap, inter = h_ref.shape
    tok, dim = xn_hbm.shape
    n_et = cap // TILE
    n_slot = weigh.shape[-1]
    n_st = n_slot // TILE
    cw = dim // n_chunk
    hw = cw // 2
    unroll = 2
    n_down = n_exp // unroll
    per_src = 4
    per_chunk = n_down + 8 // per_src
    n_steps = n_chunk * per_chunk
    slots = wdb.shape[0]
    sw = wsb.shape[-1] // 2
    n_s = wsg_ref.shape[1] // sw
    dw = wdsb.shape[-1]
    n_d = dim // dw

    def wd_copy(i):
        e, n, slot = lax.rem(i, n_exp), i // n_exp, lax.rem(i, slots)
        return pltpu.make_async_copy(wd_ref.at[e, :, pl.ds(pl.multiple_of(n * cw, cw), cw)], wdb.at[slot], wd_sem.at[slot])

    def h_copy(e):
        return pltpu.make_async_copy(h_ref.at[e], hv.at[e], hv_sem.at[e])

    def ws_copies(i):
        cols = pl.ds(pl.multiple_of(i * sw, sw), sw)
        slot = lax.rem(i, wsb.shape[0])
        return (
            pltpu.make_async_copy(wsg_ref.at[:, cols], wsb.at[slot, :, pl.ds(0, sw)], ws_sem.at[slot, 0]),
            pltpu.make_async_copy(wsu_ref.at[:, cols], wsb.at[slot, :, pl.ds(sw, sw)], ws_sem.at[slot, 1]),
        )

    def wds_copy(i):
        slot = lax.rem(i, 2)
        return pltpu.make_async_copy(wsd_ref.at[:, pl.ds(pl.multiple_of(i * dw, dw), dw)], wdsb.at[slot], wds_sem.at[slot])

    def start(copies):
        for c in copies:
            c.start()

    def wait(copies):
        for c in copies:
            c.wait()

    h_copy(0).start()
    for i in range(slots - unroll):
        wd_copy(jnp.int32(i)).start()
    for e in range(1, n_exp):
        h_copy(e).start()
    def late_copies():
        for i in range(wsb.shape[0] - 1):
            start(ws_copies(jnp.int32(i)))
        for i in range(2):
            wds_copy(jnp.int32(i)).start()
        pltpu.make_async_copy(xn_hbm, xn_ref, x_sem.at[0]).start()
        pltpu.make_async_copy(hid_hbm, hid_ref, x_sem.at[1]).start()

    barrier = pltpu.get_barrier_semaphore()
    for dev in (sib, xnb, ynb):
        pl.semaphore_signal(barrier, inc=1, device_id={"ep": dev}, device_id_type=pl.DeviceIdType.MESH)

    def build(s):
        slot = iota((tok, n_slot), 1).astype(F32)
        val = jnp.zeros((tok, n_slot), F32)
        cols = jnp.concatenate([rg_ref[s], jnp.zeros((112, 256), F32)], axis=0).T[:tok]
        for k in range(6):
            val = jnp.where(cols[:, k : k + 1] == slot, cols[:, 8 + k : 9 + k], val)
        for k, piece in enumerate(split3(val)):
            weigh[s, k * tok : (k + 1) * tok, :] = piece

    def d_copy(n):
        b = lax.rem(n, 2)
        return rcopy(part.at[b, :, 1 - core], got0.at[b], d_send.at[b], d_recv.at[b], sib)

    def p_copies(n):
        b = lax.rem(n, 4)
        return (
            rcopy(mid.at[lax.rem(n, 2), 0, :, 1 - x], got1.at[b, 0], p_send.at[b, 0], p_recv.at[b, 0], xnb),
            rcopy(mid.at[lax.rem(n, 2), 1, 1 - y], got1.at[b, 1], p_send.at[b, 1], p_recv.at[b, 1], ynb),
        )

    def q_copies(n):
        b = lax.rem(n, 4)
        return (
            rcopy(quart.at[b, 0, 1 - y], got2.at[b, 0], q_send.at[b, 0], q_recv.at[b, 0], ynb),
            rcopy(quart.at[b, 1, 1 - x], got2.at[b, 1], q_send.at[b, 1], q_recv.at[b, 1], xnb),
        )

    def stage_p(n):
        b = lax.rem(n, 2)
        d_copy(n).wait()
        for hf in range(2):
            for yy in range(2):
                for xx in range(2):
                    rows = pl.ds((yy * 2 + xx) * tok, tok)
                    mid[b, hf, yy, xx] = part[b, hf, core, rows, :] + got0[b, hf, rows, :]
        start(p_copies(n))

    def stage_q(n):
        b = lax.rem(n, 4)
        wait(p_copies(n))
        for k in range(2):
            quart[b, 0, k] = mid[lax.rem(n, 2), 0, k, x] + got1[b, 0, k]
            quart[b, 1, k] = mid[lax.rem(n, 2), 1, y, k] + got1[b, 1, k]
        start(q_copies(n))

    def stage_f(n):
        b = lax.rem(n, 4)
        wait(q_copies(n))
        total[n, 0] = quart[b, 0, y] + got2[b, 0]
        total[n, 1] = quart[b, 1, x] + got2[b, 1]

    def down(n, j):
        i0 = n * n_exp + j * unroll
        for u in range(unroll):
            i = i0 + slots - unroll + u

            @pl.when(i < n_chunk * n_exp)
            def _():
                wd_copy(i).start()

        for u in range(unroll):
            wd_copy(i0 + u).wait()

        def products():
            for u in range(unroll):
                e = j * unroll + u
                res = dot_f32(hv[e], wdb[lax.rem(i0 + u, slots)]).astype(BF16)
                etile[pl.ds(e * n_et, n_et)] = res.reshape(n_et, TILE, cw)

        @pl.when(n == 0)
        def _():
            for u in range(unroll):
                h_copy(j * unroll + u).wait()
            products()
            for u in range(8 // n_down):
                build(j * (8 // n_down) + u)

        pl.when(n > 0)(products)

    def combine(n, g):
        b = lax.rem(n, 2)
        for u in range(per_src):
            s = (g + 1 - core - 2 * g * (1 - core)) * per_src + u
            for t in range(n_st):
                esrc[u, t * TILE : (t + 1) * TILE, :] = etile[back_ref[0, s * 64 + t]]
        for u in range(per_src):
            s = (g + 1 - core - 2 * g * (1 - core)) * per_src + u
            res = dot_f32(weigh[s], esrc[u])
            res = res[:tok] + (res[tok : 2 * tok] + res[2 * tok :])
            for hf in range(2):
                part[b, hf, s // 4, u * tok : (u + 1) * tok, :] = res[:, hf * hw : (hf + 1) * hw]

    def shared_up(i):
        ahead = i + wsb.shape[0] - 1

        @pl.when(ahead < n_s)
        def _():
            start(ws_copies(ahead))

        wait(ws_copies(i))
        both = dot_f32(xn_ref[...], wsb[lax.rem(i, wsb.shape[0])])
        hs[i] = (jax.nn.silu(both[:, :sw]) * both[:, sw:]).astype(BF16)

    def step(s, carry):
        n, j = s // per_chunk, lax.rem(s, per_chunk)
        pl.when(j < n_down)(lambda: down(n, j))
        pl.when(j >= n_down)(lambda: combine(n, j - n_down))
        pl.when((n == 1) & (j == n_down))(late_copies)
        @pl.when(j == n_down)
        def _():
            pl.when(n == 0)(lambda: pl.semaphore_wait(barrier, 3))
            d_copy(n).start()

        @pl.when(j == 0)
        def _():
            pl.when(n >= 1)(lambda: stage_p(n - 1))
            pl.when(n >= 4)(lambda: stage_f(n - 4))

        pl.when((j == n_down) & (n >= 2))(lambda: stage_q(n - 2))

        return carry

    lax.fori_loop(0, n_steps, step, 0)

    last = jnp.int32(n_chunk - 1)

    def up_step(i, carry):
        shared_up(i)
        pl.when(i == 0)(lambda: stage_p(last))
        pl.when(i == 4)(lambda: stage_q(last - 1))

        @pl.when(i == 8)
        def _():
            stage_f(last - 3)
            stage_f(last - 2)

        return carry

    pltpu.make_async_copy(xn_hbm, xn_ref, x_sem.at[0]).wait()
    pltpu.make_async_copy(hid_hbm, hid_ref, x_sem.at[1]).wait()
    lax.fori_loop(0, n_s, up_step, 0)
    for i in range(n_d):
        wds_copy(jnp.int32(i)).wait()
        res = jnp.zeros((tok, dw), F32)
        for k in range(n_s):
            res = res + dot_f32(hs[k], wdsb[i % 2, k * sw : (k + 1) * sw, :])
        out_ref[:, i * dw : (i + 1) * dw] = res.astype(BF16)
        if i + 2 < n_d:
            wds_copy(jnp.int32(i + 2)).start()
        if i == 1:
            stage_q(last)
    stage_f(last - 1)
    stage_f(last)
    for n in range(n_chunk):
        for hf in range(2):
            cols = slice(n * cw + hf * hw, n * cw + (hf + 1) * hw)
            out_ref[:, cols] = (hid_ref[:, cols].astype(F32) + out_ref[:, cols].astype(F32) + total[n, hf]).astype(BF16)


def solution(mesh):
    ep_size = mesh.shape["ep"]
    assert ep_size == 8

    def local_block(hidden_in, norm_gain, router_w, w_gate, w_up, w_down, ws_gate, ws_up, ws_down, expert_ids):
        tok, top_k = expert_ids.shape
        dim = hidden_in.shape[1]
        n_exp, _, inter = w_gate.shape
        s_inter = ws_gate.shape[1]
        cap = GROUPS * ((top_k + GROUP_LIMIT - 1) // GROUP_LIMIT) * tok // n_exp
        n_kc, slots = 4, 3
        kw = dim // n_kc
        pair_cap = cap * n_exp // ep_size
        n_st = (pair_cap + 14 * n_exp) // TILE + n_exp
        n_slot = -(-(n_st + 1) * TILE // 128) * 128
        n_st = n_slot // TILE
        assert n_st <= 64
        vmem = pl.BlockSpec(memory_space=pltpu.VMEM)
        smem = pl.BlockSpec(memory_space=pltpu.SMEM)
        hbm = pl.BlockSpec(memory_space=pl.ANY)
        dma = pltpu.SemaphoreType.DMA
        h, rg, xn, _, back = pl.pallas_call(
            functools.partial(gather_up_kernel, n_kc),
            out_shape=(
                jax.ShapeDtypeStruct((n_exp, cap, inter), BF16),
                jax.ShapeDtypeStruct((8, 16, 256), F32),
                jax.ShapeDtypeStruct((tok, dim), BF16),
                jax.ShapeDtypeStruct((n_exp, 256), jnp.int32),
                jax.ShapeDtypeStruct((1, 512), jnp.int32),
            ),
            in_specs=[vmem, vmem, vmem, vmem, hbm, hbm],
            out_specs=(hbm, vmem, hbm, hbm, vmem),
            scratch_shapes=[
                pltpu.VMEM((n_kc, 8 * tok, kw), BF16),
                pltpu.VMEM((8, n_slot, tok), BF16),
                pltpu.VMEM((7 * n_st + 64, TILE, kw), BF16),
                pltpu.VMEM((n_exp, cap, 2 * inter), F32),
                pltpu.VMEM((slots, kw, 2 * inter), BF16),
                pltpu.VMEM((2, cap, inter), BF16),
                pltpu.VMEM((2, cap, kw), BF16),
                pltpu.VMEM((8, n_exp, 256), F32),
                pltpu.VMEM((8, n_exp, 256), F32),
                pltpu.VMEM((8, 8, 256), jnp.int32),
                pltpu.VMEM((n_exp, 256), jnp.int32),
                pltpu.SMEM((n_exp, 256), jnp.int32),
                pltpu.VMEM((8, 8, 256), F32),
                pltpu.VMEM((8, 256), jnp.int32),
                dma((slots, 2)),
                dma((2,)),
                dma((2,)),
                dma((n_kc,)),
                dma((8,)),
                dma((8,)),
                dma((8,)),
                dma((8,)),
                dma((n_kc, 11)),
                dma((n_kc, 11)),
            ],
            compiler_params=pltpu.CompilerParams(collective_id=0, has_side_effects=True, vmem_limit_bytes=VMEM_LIMIT),
            name="gather_up",
        )(hidden_in, norm_gain.reshape(1, dim), router_w, expert_ids.T, w_gate, w_up)

        n_chunk, dslots = 8, 12
        cw = dim // n_chunk
        hw = cw // 2
        sw, dw = 256, 512
        return pl.pallas_call(
            functools.partial(down_kernel, n_chunk),
            out_shape=jax.ShapeDtypeStruct((tok, dim), BF16),
            in_specs=[vmem, smem, hbm, hbm, hbm, hbm, hbm, hbm, hbm],
            out_specs=vmem,
            scratch_shapes=[
                pltpu.VMEM((n_exp, cap, inter), BF16),
                pltpu.VMEM((8, 3 * tok, n_slot), BF16),
                pltpu.VMEM((dslots, inter, cw), BF16),
                pltpu.VMEM((n_exp * cap // TILE, TILE, cw), BF16),
                pltpu.VMEM((4, n_slot, cw), BF16),
                pltpu.VMEM((2, 2, 2, 4 * tok, hw), F32),
                pltpu.VMEM((2, 2, 4 * tok, hw), F32),
                pltpu.VMEM((2, 2, 2, 2, tok, hw), F32),
                pltpu.VMEM((4, 2, 2, tok, hw), F32),
                pltpu.VMEM((4, 2, 2, tok, hw), F32),
                pltpu.VMEM((4, 2, tok, hw), F32),
                pltpu.VMEM((n_chunk, 2, tok, hw), F32),
                pltpu.VMEM((5, dim, 2 * sw), BF16),
                pltpu.VMEM((2, s_inter, dw), BF16),
                pltpu.VMEM((s_inter // sw, tok, sw), BF16),
                pltpu.VMEM((tok, dim), BF16),
                pltpu.VMEM((tok, dim), BF16),
                dma((2,)),
                dma((n_exp,)),
                dma((dslots,)),
                dma((5, 2)),
                dma((2,)),
                dma((2,)),
                dma((2,)),
                dma((4, 2)),
                dma((4, 2)),
                dma((4, 2)),
                dma((4, 2)),
            ],
            compiler_params=pltpu.CompilerParams(collective_id=1, has_side_effects=True, vmem_limit_bytes=VMEM_LIMIT),
            name="down_sum",
        )(rg, back, hidden_in, xn, h, w_down, ws_gate, ws_up, ws_down)

    row_spec = P(("dp", "ep"), None)
    in_specs = (row_spec, P(), P(), P("ep"), P("ep"), P("ep"), P(), P(), P(), row_spec)
    return jax.shard_map(local_block, mesh=mesh, in_specs=in_specs, out_specs=row_spec, check_vma=False)
```
